32 devices in a mesh: blk: 16 (over z, y, core), uly: 2 (over x).
Axes of the slice: x: 2, y: 2, z: 4, core: 2. Of those that a mesh axis runs over, the one named last changes fastest.
Arguments:
- footage_probes: bfloat16 [1024, 32, 64], P(('blk', 'uly')), may hold values from -6 to 6
- footage_lookup_keys: bfloat16 [1024, 32, 64], P(('blk', 'uly')), may hold values from -6 to 6
- footage_payload: bfloat16 [1024, 32, 64], P(('blk', 'uly')), may hold values from -6 to 6
- caption_probes: bfloat16 [256, 32, 64], replicated, may hold values from -6 to 6
- caption_lookup_keys: bfloat16 [256, 32, 64], replicated, may hold values from -6 to 6
- caption_payload: bfloat16 [256, 32, 64], replicated, may hold values from -6 to 6
- footage_probes_amplitude: float32 [64], replicated, may hold values from 0.25 to 1.75
- footage_keys_amplitude: float32 [64], replicated, may hold values from 0.25 to 1.75
- caption_probes_amplitude: float32 [64], replicated, may hold values from 0.25 to 1.75
- caption_keys_amplitude: float32 [64], replicated, may hold values from 0.25 to 1.75
- focus_sharpness: float32 [32], replicated, may hold values from 1.5 to 4
- caption_validity: int32 [256], replicated, may hold values 0 or 1
Outputs:
- vid_out: bfloat16 [1024, 32, 64], P(('blk', 'uly'))
- txt_out: bfloat16 [256, 32, 64], P('uly', 'blk')
The draws below stay inside these ranges and needn't reach their ends.
Inputs may be any that keep to these rules, and one draw needn't show every extreme that they name: caption_validity holds only 0 and 1.
All inputs are finite; a program needn't handle non-finite values.
Results may differ from the reference program's by a relative error of at most 0.0035.
Values may be sent and summed in bfloat16 or wider, within the bound.
A program may use at most 64 MiB of HBM per device.

```python
import math
import jax
import jax.numpy as jnp
from jax import lax

FOCUS_COUNT = 32
WIDTH_EACH = 64
TTOK = 256
VTOK = 1024


def place_ends(entries, rng, smallest, top_value):
    place = [jax.random.randint(jax.random.fold_in(rng, axis), (), 0, length) for axis, length in enumerate(entries.shape)]
    widest = entries.shape.index(max(entries.shape))
    beside = place[:widest] + [(place[widest] + 1) % entries.shape[widest]] + place[widest + 1:]
    return entries.at[tuple(place)].set(smallest).at[tuple(beside)].set(top_value)


def level_of(own_key, shape, shards, smallest, largest):
    gain = 1.0
    for dim, parts in shards:
        heights = jax.random.uniform(jax.random.fold_in(jax.random.fold_in(own_key, 6), dim), (parts,), jnp.float32, smallest / len(shards), largest / len(shards))
        gain = gain * jnp.repeat(jnp.exp(heights), shape[dim] // parts).reshape((-1,) + (1,) * (len(shape) - 1 - dim))
    return gain


def gaussian(key, dims, spread, limit, pieces=(), kind=jnp.bfloat16):
    result = jax.random.normal(key, dims, jnp.float32) * spread
    if len(pieces) > 0:
        result = level_of(key, dims, pieces, -0.22, 0.18) * result
    return jnp.clip(result, min=-limit, max=limit).astype(kind)


def setup_inputs(seed: int = 0) -> dict:
    splits = jax.random.split(jax.random.key(seed), 13)
    return {
        "footage_probes": gaussian(splits[0], (VTOK, FOCUS_COUNT, WIDTH_EACH), 1.0, 6.0, ((0, 32),)),
        "footage_lookup_keys": gaussian(splits[1], (VTOK, FOCUS_COUNT, WIDTH_EACH), 1.0, 6.0, ((0, 32),)),
        "footage_payload": gaussian(splits[2], (VTOK, FOCUS_COUNT, WIDTH_EACH), 1.0, 6.0, ((0, 32),)),
        "caption_probes": gaussian(splits[3], (TTOK, FOCUS_COUNT, WIDTH_EACH), 1.0, 6.0),
        "caption_lookup_keys": gaussian(splits[4], (TTOK, FOCUS_COUNT, WIDTH_EACH), 1.0, 6.0),
        "caption_payload": gaussian(splits[5], (TTOK, FOCUS_COUNT, WIDTH_EACH), 1.0, 6.0),
        "footage_probes_amplitude": jnp.clip(1.0 + 0.15 * jax.random.normal(splits[6], (WIDTH_EACH,), jnp.float32), 0.25, 1.75),
        "footage_keys_amplitude": jnp.clip(1.0 + 0.15 * jax.random.normal(splits[7], (WIDTH_EACH,), jnp.float32), 0.25, 1.75),
        "caption_probes_amplitude": jnp.clip(1.0 + 0.15 * jax.random.normal(splits[8], (WIDTH_EACH,), jnp.float32), 0.25, 1.75),
        "caption_keys_amplitude": jnp.clip(1.0 + 0.15 * jax.random.normal(splits[9], (WIDTH_EACH,), jnp.float32), 0.25, 1.75),
        "focus_sharpness": jnp.clip(jnp.exp(jax.random.uniform(splits[10], (FOCUS_COUNT,), jnp.float32, math.log(1.5), math.log(4.0))), 1.5, 4.0),
        "caption_validity": place_ends((jax.random.randint(splits[11], (TTOK,), 0, 8) < 7).astype(jnp.int32), jax.random.fold_in(splits[11], 1), 0, 1),
    }


EPSILON = 1e-06

def normed(tensor, gain_vector, rescale_factor):
    widened = tensor.astype(jnp.float32)
    inverse = lax.rsqrt(lax.optimization_barrier(jnp.mean(widened * widened, axis=-1, keepdims=True)) + EPSILON)
    return (widened * inverse * gain_vector * rescale_factor).astype(jnp.bfloat16)

def reference(footage_probes, footage_lookup_keys, footage_payload, caption_probes, caption_lookup_keys, caption_payload, footage_probes_amplitude, footage_keys_amplitude, caption_probes_amplitude, caption_keys_amplitude, focus_sharpness, caption_validity):
    rescale_factor = focus_sharpness[None, :, None] / math.sqrt(WIDTH_EACH)
    queries = jnp.concatenate([normed(footage_probes, footage_probes_amplitude, rescale_factor), normed(caption_probes, caption_probes_amplitude, rescale_factor)], 0)
    key_rows = jnp.concatenate([normed(footage_lookup_keys, footage_keys_amplitude, 1.0), normed(caption_lookup_keys, caption_keys_amplitude, 1.0)], 0)
    value_rows = jnp.concatenate([footage_payload, caption_payload], 0)
    key_valid = jnp.concatenate([jnp.ones((VTOK,), dtype=bool), caption_validity == 1], 0)

    def one_head(argument_bundle):
        query_head, key_head, value_head = argument_bundle
        scores = jnp.dot(query_head.astype(jnp.float32), key_head.astype(jnp.float32).T, precision=lax.Precision.HIGHEST)
        scores = jnp.where(key_valid[None, :], scores, -jnp.inf)
        weights = jax.nn.softmax(scores, axis=-1)
        return jnp.dot(weights, value_head.astype(jnp.float32), precision=lax.Precision.HIGHEST).astype(jnp.bfloat16)
    attended = lax.map(one_head, (jnp.transpose(queries, (1, 0, 2)), jnp.transpose(key_rows, (1, 0, 2)), jnp.transpose(value_rows, (1, 0, 2))))
    attended = jnp.transpose(attended, (1, 0, 2))
    return (attended[:VTOK], attended[VTOK:])
```

```python
import functools
import math

import jax
import jax.numpy as jnp
from jax import lax
from jax.experimental import pallas as pl
from jax.experimental.pallas import tpu as pltpu
from jax.sharding import PartitionSpec as P

EPSILON = 1e-06
NEGATIVE = -1e30
MESH = pl.DeviceIdType.MESH


def normed(tensor, gain_vector, rescale_factor):
    widened = tensor.astype(jnp.float32)
    inverse = lax.rsqrt(jnp.mean(widened * widened, axis=-1, keepdims=True) + EPSILON)
    return (widened * inverse * gain_vector * rescale_factor).astype(jnp.bfloat16)


def fragment_contributions(queries, key_rows, value_rows, valid):
    scores = jnp.einsum("qhd,khd->hqk", queries, key_rows, preferred_element_type=jnp.float32)
    if valid is not None:
        scores = jnp.where(valid[None, None, :], scores, NEGATIVE)
    maxima = jnp.max(scores, axis=-1)
    weights = jnp.exp(scores - maxima[..., None])
    if valid is not None:
        weights = jnp.where(valid[None, None, :], weights, 0.0)
    totals = jnp.sum(weights, axis=-1)
    accum = jnp.einsum(
        "hqk,khd->hqd", weights, value_rows.astype(jnp.float32), precision=lax.Precision.HIGHEST
    )
    return (maxima, totals, accum)


def combine(earlier, later):
    max_one, total_one, accum_one = earlier
    max_two, total_two, accum_two = later
    merged_max = jnp.maximum(max_one, max_two)
    factor_one = jnp.exp(max_one - merged_max)
    factor_two = jnp.exp(max_two - merged_max)
    merged_total = total_one * factor_one + total_two * factor_two
    merged_accum = accum_one * factor_one[..., None] + accum_two * factor_two[..., None]
    return (merged_max, merged_total, merged_accum)


def on_device(
    footage_probes,
    footage_lookup_keys,
    footage_payload,
    caption_probes,
    caption_lookup_keys,
    caption_payload,
    footage_probes_amplitude,
    footage_keys_amplitude,
    caption_probes_amplitude,
    caption_keys_amplitude,
    focus_sharpness,
    caption_validity,
):
    channel_width = footage_probes.shape[2]
    rescale_factor = focus_sharpness[None, :, None] / math.sqrt(channel_width)
    q_norm = normed(footage_probes, footage_probes_amplitude, rescale_factor)
    k_norm = normed(footage_lookup_keys, footage_keys_amplitude, 1.0)
    q_local = lax.all_to_all(q_norm, "blk", split_axis=1, concat_axis=0, tiled=True)
    k_local = lax.all_to_all(k_norm, "blk", split_axis=1, concat_axis=0, tiled=True)
    v_local = lax.all_to_all(footage_payload, "blk", split_axis=1, concat_axis=0, tiled=True)
    local_heads = q_local.shape[1]
    head_start = lax.axis_index("blk") * local_heads
    local_scale = lax.dynamic_slice_in_dim(rescale_factor, head_start, local_heads, 1)
    text_q = normed(
        lax.dynamic_slice_in_dim(caption_probes, head_start, local_heads, 1),
        caption_probes_amplitude,
        local_scale,
    )
    text_k = normed(
        lax.dynamic_slice_in_dim(caption_lookup_keys, head_start, local_heads, 1),
        caption_keys_amplitude,
        1.0,
    )
    text_v = lax.dynamic_slice_in_dim(caption_payload, head_start, local_heads, 1)
    text_valid = caption_validity == 1
    text_share = caption_probes.shape[0] // lax.axis_size("uly")
    row_start = lax.axis_index("uly") * text_share
    video_rows = q_local.shape[0]
    queries = jnp.concatenate(
        [q_local, lax.dynamic_slice_in_dim(text_q, row_start, text_share, 0)], 0
    )

    def fold_inward(running, gathered):
        key_block, value_block = gathered
        row_count = key_block.shape[0]
        block_rows = math.gcd(row_count, 512)

        def absorb_block(block_index, running_state):
            key_part = lax.dynamic_slice_in_dim(key_block, block_index * block_rows, block_rows, 0)
            value_part = lax.dynamic_slice_in_dim(
                value_block, block_index * block_rows, block_rows, 0
            )
            return combine(
                running_state, fragment_contributions(queries, key_part, value_part, None)
            )

        return lax.fori_loop(0, row_count // block_rows, absorb_block, running)

    first_state = fragment_contributions(queries, text_k, text_v, text_valid)
    maxima, totals, accum = fold_inward(
        first_state,
        (
            lax.all_gather(k_local, "uly", axis=0, tiled=True),
            lax.all_gather(v_local, "uly", axis=0, tiled=True),
        ),
    )
    attended = jnp.transpose(accum / totals[..., None], (1, 0, 2)).astype(jnp.bfloat16)
    vid_out = lax.all_to_all(attended[:video_rows], "blk", split_axis=0, concat_axis=1, tiled=True)
    txt_out = attended[video_rows:]
    return (vid_out, txt_out)


def peer_id(flat, uly_count):
    return {"blk": flat // uly_count, "uly": flat % uly_count}


def lane_mask(shape, half):
    return lax.broadcasted_iota(jnp.int32, shape, len(shape) - 1) < half


def unit_rows(rows):
    return rows * lax.rsqrt(jnp.mean(rows * rows, axis=-1, keepdims=True) + EPSILON)


def fused_kernel(
    blk_count,
    uly_count,
    vq_hbm,
    vk_hbm,
    vv_hbm,
    tq_hbm,
    tk_hbm,
    tv_hbm,
    vq_gain,
    vk_gain,
    tq_gain,
    tk_gain,
    sharp,
    valid,
    vid_out,
    txt_out,
    vq_in,
    vk_in,
    vv_in,
    tq_in,
    tk_in,
    tv_in,
    kv_wide,
    q_wide,
    text_wide,
    send,
    recv,
    text_kv,
    values,
    text_q,
    back_send,
    back_recv,
    back_wide,
    text_send,
    text_recv,
    text_out_wide,
    in_sem,
    send_sem,
    recv_sem,
    back_send_sem,
    back_recv_sem,
    text_send_sem,
    text_recv_sem,
):
    count = blk_count * uly_count
    my_blk = lax.axis_index("blk")
    my_uly = lax.axis_index("uly")
    me = my_blk * uly_count + my_uly
    tokens, heads, width = vq_in.shape
    half_tokens = tokens // 2
    text_tokens, band, _ = tq_in.shape
    text_share = text_tokens // uly_count
    lanes = 2 * width

    barrier = pltpu.get_barrier_semaphore()

    def greet(step, carry):
        peer = (me + 1 + step) % count
        pl.semaphore_signal(
            barrier, inc=1, device_id=peer_id(peer, uly_count), device_id_type=MESH
        )
        return carry

    lax.fori_loop(0, count - 1, greet, 0)

    band_start = pl.multiple_of(me // band * band, band)
    loads = []
    for slot, (source, target) in enumerate(
        ((vk_hbm, vk_in), (vv_hbm, vv_in), (vq_hbm, vq_in))
    ):
        loads.append(pltpu.make_async_copy(source, target, in_sem.at[slot]))
    for slot, (source, target) in enumerate(
        ((tk_hbm, tk_in), (tv_hbm, tv_in), (tq_hbm, tq_in))
    ):
        loads.append(
            pltpu.make_async_copy(
                source.at[:, pl.ds(band_start, band), :], target, in_sem.at[3 + slot]
            )
        )
    for load in loads:
        load.start()

    sharp_row = sharp[...] / math.sqrt(width)
    square = (heads, heads)
    sharp_column = jnp.sum(
        jnp.where(
            lax.broadcasted_iota(jnp.int32, square, 0) == lax.broadcasted_iota(jnp.int32, square, 1),
            jnp.broadcast_to(sharp_row, square),
            0.0,
        ),
        axis=1,
        keepdims=True,
    )
    my_sharp = jnp.sum(
        jnp.where(lax.broadcasted_iota(jnp.int32, (1, heads), 1) == me, sharp_row, 0.0),
        axis=1,
        keepdims=True,
    )

    loads[0].wait()
    loads[1].wait()
    keys = unit_rows(vk_in[...].astype(jnp.float32)) * vk_gain[...][None]
    kv_wide[...] = jnp.concatenate([keys, vv_in[...].astype(jnp.float32)], axis=-1)
    loads[2].wait()
    probes = unit_rows(vq_in[...].astype(jnp.float32)) * vq_gain[...][None] * sharp_column[None]
    q_wide[...] = jnp.concatenate([probes[:half_tokens], probes[half_tokens:]], axis=-1)
    for head in range(heads):
        send[head, :tokens, :] = kv_wide[:, head, :].astype(jnp.bfloat16)
        send[head, tokens:, :] = q_wide[:, head, :].astype(jnp.bfloat16)
    recv[me] = send[me]

    pl.semaphore_wait(barrier, count - 1)

    def outward(peer):
        return pltpu.make_async_remote_copy(
            src_ref=send.at[peer],
            dst_ref=recv.at[me],
            send_sem=send_sem.at[peer],
            recv_sem=recv_sem.at[me],
            device_id=peer_id(peer, uly_count),
            device_id_type=MESH,
        )

    def inward(peer):
        return pltpu.make_async_remote_copy(
            src_ref=send.at[peer],
            dst_ref=recv.at[peer],
            send_sem=send_sem.at[peer],
            recv_sem=recv_sem.at[peer],
            device_id=peer_id(peer, uly_count),
            device_id_type=MESH,
        )

    def dispatch(step, carry):
        distance = count // 2 + (1 - 2 * (step % 2)) * ((step + 1) // 2)
        outward((me + distance) % count).start()
        return carry

    lax.fori_loop(0, count - 1, dispatch, 0)

    my_row = me % band
    loads[3].wait()
    text_wide[...] = tk_in[...].astype(jnp.float32)
    text_keys = unit_rows(text_wide[:, my_row, :]) * tk_gain[...]
    loads[4].wait()
    text_wide[...] = tv_in[...].astype(jnp.float32)
    both = jnp.concatenate([text_keys, text_wide[:, my_row, :]], axis=-1)
    text_kv[...] = both.astype(jnp.bfloat16)
    video_tokens = count * tokens
    values[video_tokens:, :] = jnp.where(lane_mask(both.shape, width), 1.0, both).astype(
        jnp.bfloat16
    )
    loads[5].wait()
    text_wide[...] = tq_in[...].astype(jnp.float32)
    text_probes = unit_rows(text_wide[:, my_row, :]) * tq_gain[...] * my_sharp
    text_q[...] = jnp.concatenate([text_probes, jnp.zeros_like(text_probes)], axis=-1).astype(
        jnp.bfloat16
    )
    bias = jnp.where(valid[...] == 1, 0.0, NEGATIVE)

    def arrive(step, carry):
        inward((me + 1 + step) % count).wait_recv()
        return carry

    lax.fori_loop(0, count - 1, arrive, 0)

    video_kv = recv[:, :tokens, :].reshape(video_tokens, lanes)
    values[:video_tokens, :] = jnp.where(
        lane_mask(video_kv.shape, width), 1.0, video_kv.astype(jnp.float32)
    ).astype(jnp.bfloat16)

    def attend(rows):
        video_scores = lax.dot_general(
            rows,
            recv[:, :tokens, :].reshape(video_tokens, lanes),
            (((1,), (1,)), ((), ())),
            preferred_element_type=jnp.float32,
        )
        text_scores = (
            lax.dot_general(
                rows,
                text_kv[...],
                (((1,), (1,)), ((), ())),
                preferred_element_type=jnp.float32,
            )
            + bias
        )
        peak = jnp.maximum(
            jnp.max(video_scores, axis=1, keepdims=True),
            jnp.max(text_scores, axis=1, keepdims=True),
        )
        video_weights = jnp.exp(video_scores - peak).astype(jnp.bfloat16)
        text_weights = jnp.exp(text_scores - peak).astype(jnp.bfloat16)
        total = jnp.dot(
            video_weights, values[:video_tokens, :], preferred_element_type=jnp.float32
        ) + jnp.dot(text_weights, values[video_tokens:, :], preferred_element_type=jnp.float32)
        return total / pltpu.roll(total, width, 1)

    def pair_up(first, second):
        return jnp.where(lane_mask(first.shape, width), pltpu.roll(first, width, 1), second)

    def homeward(peer):
        return pltpu.make_async_remote_copy(
            src_ref=back_send.at[peer],
            dst_ref=back_recv.at[me],
            send_sem=back_send_sem.at[peer],
            recv_sem=back_recv_sem.at[me],
            device_id=peer_id(peer, uly_count),
            device_id_type=MESH,
        )

    def returned(peer):
        return pltpu.make_async_remote_copy(
            src_ref=back_send.at[peer],
            dst_ref=back_recv.at[peer],
            send_sem=back_send_sem.at[peer],
            recv_sem=back_recv_sem.at[peer],
            device_id=peer_id(peer, uly_count),
            device_id_type=MESH,
        )

    group = math.gcd(count, 8)
    group_count = count // group
    group_rows = group * half_tokens

    def video_group(step, carry):
        which = (me // group + group_count // 2 + step) % group_count
        first_peer = pl.multiple_of(which * group, group)
        packed = (
            recv[pl.ds(first_peer, group), tokens:, :]
            .reshape(group_rows, lanes)
            .astype(jnp.float32)
        )
        low = lane_mask(packed.shape, width)
        rows = jnp.concatenate(
            [jnp.where(low, packed, 0.0), jnp.where(low, pltpu.roll(packed, width, 1), 0.0)], axis=0
        ).astype(jnp.bfloat16)
        attended = attend(rows)
        back_send[pl.ds(first_peer, group)] = (
            pair_up(attended[:group_rows], attended[group_rows:])
            .astype(jnp.bfloat16)
            .reshape(group, half_tokens, lanes)
        )

        def hand_back(index, inner):
            peer = first_peer + (index + me) % group

            @pl.when(peer != me)
            def _():
                homeward(peer).start()

            return inner

        lax.fori_loop(0, group, hand_back, 0)
        return carry

    lax.fori_loop(0, group_count, video_group, 0)
    back_recv[me] = back_send[me]

    attended = attend(text_q[...])
    half_share = text_share // 2
    for part in range(uly_count):
        base = part * text_share
        text_send[part] = pair_up(
            attended[base : base + half_share], attended[base + half_share : base + text_share]
        ).astype(jnp.bfloat16)

    def text_copy(part, slot):
        return pltpu.make_async_remote_copy(
            src_ref=text_send.at[part],
            dst_ref=text_recv.at[slot],
            send_sem=text_send_sem.at[part],
            recv_sem=text_recv_sem.at[slot],
            device_id={"blk": my_blk, "uly": part},
            device_id_type=MESH,
        )

    for step in range(1, uly_count):
        text_copy((my_uly + step) % uly_count, my_uly).start()
    text_recv[my_uly] = text_send[my_uly]

    for step in range(1, uly_count):
        other = (my_uly + step) % uly_count
        text_copy(other, other).wait_recv()
    for part in range(uly_count):
        block = text_recv[part].astype(jnp.float32)
        text_out_wide[:, part, :] = jnp.concatenate([block[:, :width], block[:, width:]], axis=0)
    txt_out[...] = text_out_wide[...].astype(jnp.bfloat16)

    def collect(step, carry):
        returned((me + 1 + step) % count).wait_recv()
        return carry

    lax.fori_loop(0, count - 1, collect, 0)
    for head in range(heads):
        back_wide[:, head, :] = back_recv[head].astype(jnp.float32)
    vid_out[:half_tokens] = back_wide[:, :, :width].astype(jnp.bfloat16)
    vid_out[half_tokens:] = back_wide[:, :, width:].astype(jnp.bfloat16)

    def drain(step, carry):
        peer = (me + 1 + step) % count
        outward(peer).wait_send()
        homeward(peer).wait_send()
        return carry

    lax.fori_loop(0, count - 1, drain, 0)
    for step in range(1, uly_count):
        text_copy((my_uly + step) % uly_count, my_uly).wait_send()


def fused_on_device(blk_count, uly_count, *operands):
    vq, vk, vv, tq, tk, tv, vq_gain, vk_gain, tq_gain, tk_gain, sharp, valid = operands
    tokens, heads, width = vq.shape
    text_tokens = tq.shape[0]
    count = blk_count * uly_count
    lanes = 2 * width
    text_share = text_tokens // uly_count
    band = math.gcd(heads, 8)
    half = tokens // 2
    bf16, f32 = jnp.bfloat16, jnp.float32
    any_spec = pl.BlockSpec(memory_space=pl.ANY)
    vmem_spec = pl.BlockSpec(memory_space=pltpu.VMEM)
    dma = pltpu.SemaphoreType.DMA
    return pl.pallas_call(
        functools.partial(fused_kernel, blk_count, uly_count),
        out_shape=(
            jax.ShapeDtypeStruct((tokens, heads, width), bf16),
            jax.ShapeDtypeStruct((text_share, uly_count, width), bf16),
        ),
        in_specs=[any_spec] * 6 + [vmem_spec] * 6,
        out_specs=(vmem_spec, vmem_spec),
        scratch_shapes=[
            pltpu.VMEM((tokens, heads, width), bf16),
            pltpu.VMEM((tokens, heads, width), bf16),
            pltpu.VMEM((tokens, heads, width), bf16),
            pltpu.VMEM((text_tokens, band, width), bf16),
            pltpu.VMEM((text_tokens, band, width), bf16),
            pltpu.VMEM((text_tokens, band, width), bf16),
            pltpu.VMEM((tokens, heads, lanes), f32),
            pltpu.VMEM((half, heads, lanes), f32),
            pltpu.VMEM((text_tokens, band, width), f32),
            pltpu.VMEM((count, tokens + half, lanes), bf16),
            pltpu.VMEM((count, tokens + half, lanes), bf16),
            pltpu.VMEM((text_tokens, lanes), bf16),
            pltpu.VMEM((count * tokens + text_tokens, lanes), bf16),
            pltpu.VMEM((text_tokens, lanes), bf16),
            pltpu.VMEM((count, half, lanes), bf16),
            pltpu.VMEM((count, half, lanes), bf16),
            pltpu.VMEM((half, heads, lanes), f32),
            pltpu.VMEM((uly_count, text_share // 2, lanes), bf16),
            pltpu.VMEM((uly_count, text_share // 2, lanes), bf16),
            pltpu.VMEM((text_share, uly_count, width), f32),
            dma((6,)),
            dma((count,)),
            dma((count,)),
            dma((count,)),
            dma((count,)),
            dma((uly_count,)),
            dma((uly_count,)),
        ],
        compiler_params=pltpu.CompilerParams(collective_id=0, has_side_effects=True),
        name="joint_attention",
    )(
        vq,
        vk,
        vv,
        tq,
        tk,
        tv,
        vq_gain[None],
        vk_gain[None],
        tq_gain[None],
        tk_gain[None],
        sharp[None],
        valid[None],
    )


def fits_fused(mesh, vq, tq):
    count = mesh.shape["blk"] * mesh.shape["uly"]
    tokens = vq.shape[0] // count
    return (
        vq.shape[1] == count
        and 2 * vq.shape[2] == 128
        and tokens % 32 == 0
        and tokens <= 64
        and tq.shape[0] % (32 * mesh.shape["uly"]) == 0
    )


def solution(mesh):
    blk_count, uly_count = mesh.shape["blk"], mesh.shape["uly"]

    def run(*operands):
        body = on_device
        if fits_fused(mesh, operands[0], operands[3]):
            body = functools.partial(fused_on_device, blk_count, uly_count)
        split = P(("blk", "uly"), None, None)
        return jax.shard_map(
            body,
            mesh=mesh,
            in_specs=(split, split, split) + (P(),) * 9,
            out_specs=(split, P("uly", "blk", None)),
            check_vma=False,
        )(*operands)

    return run
```

```python
import functools
import math

import jax
import jax.numpy as jnp
from jax import lax
from jax.experimental import pallas as pl
from jax.experimental.pallas import tpu as pltpu
from jax.sharding import PartitionSpec as P

EPSILON = 1e-06
NEGATIVE = -1e30
MESH = pl.DeviceIdType.MESH


def normed(tensor, gain_vector, rescale_factor):
    widened = tensor.astype(jnp.float32)
    inverse = lax.rsqrt(jnp.mean(widened * widened, axis=-1, keepdims=True) + EPSILON)
    return (widened * inverse * gain_vector * rescale_factor).astype(jnp.bfloat16)


def fragment_contributions(queries, key_rows, value_rows, valid):
    scores = jnp.einsum("qhd,khd->hqk", queries, key_rows, preferred_element_type=jnp.float32)
    if valid is not None:
        scores = jnp.where(valid[None, None, :], scores, NEGATIVE)
    maxima = jnp.max(scores, axis=-1)
    weights = jnp.exp(scores - maxima[..., None])
    if valid is not None:
        weights = jnp.where(valid[None, None, :], weights, 0.0)
    totals = jnp.sum(weights, axis=-1)
    accum = jnp.einsum(
        "hqk,khd->hqd", weights, value_rows.astype(jnp.float32), precision=lax.Precision.HIGHEST
    )
    return (maxima, totals, accum)


def combine(earlier, later):
    max_one, total_one, accum_one = earlier
    max_two, total_two, accum_two = later
    merged_max = jnp.maximum(max_one, max_two)
    factor_one = jnp.exp(max_one - merged_max)
    factor_two = jnp.exp(max_two - merged_max)
    merged_total = total_one * factor_one + total_two * factor_two
    merged_accum = accum_one * factor_one[..., None] + accum_two * factor_two[..., None]
    return (merged_max, merged_total, merged_accum)


def on_device(
    footage_probes,
    footage_lookup_keys,
    footage_payload,
    caption_probes,
    caption_lookup_keys,
    caption_payload,
    footage_probes_amplitude,
    footage_keys_amplitude,
    caption_probes_amplitude,
    caption_keys_amplitude,
    focus_sharpness,
    caption_validity,
):
    channel_width = footage_probes.shape[2]
    rescale_factor = focus_sharpness[None, :, None] / math.sqrt(channel_width)
    q_norm = normed(footage_probes, footage_probes_amplitude, rescale_factor)
    k_norm = normed(footage_lookup_keys, footage_keys_amplitude, 1.0)
    q_local = lax.all_to_all(q_norm, "blk", split_axis=1, concat_axis=0, tiled=True)
    k_local = lax.all_to_all(k_norm, "blk", split_axis=1, concat_axis=0, tiled=True)
    v_local = lax.all_to_all(footage_payload, "blk", split_axis=1, concat_axis=0, tiled=True)
    local_heads = q_local.shape[1]
    head_start = lax.axis_index("blk") * local_heads
    local_scale = lax.dynamic_slice_in_dim(rescale_factor, head_start, local_heads, 1)
    text_q = normed(
        lax.dynamic_slice_in_dim(caption_probes, head_start, local_heads, 1),
        caption_probes_amplitude,
        local_scale,
    )
    text_k = normed(
        lax.dynamic_slice_in_dim(caption_lookup_keys, head_start, local_heads, 1),
        caption_keys_amplitude,
        1.0,
    )
    text_v = lax.dynamic_slice_in_dim(caption_payload, head_start, local_heads, 1)
    text_valid = caption_validity == 1
    text_share = caption_probes.shape[0] // lax.axis_size("uly")
    row_start = lax.axis_index("uly") * text_share
    video_rows = q_local.shape[0]
    queries = jnp.concatenate(
        [q_local, lax.dynamic_slice_in_dim(text_q, row_start, text_share, 0)], 0
    )

    def fold_inward(running, gathered):
        key_block, value_block = gathered
        row_count = key_block.shape[0]
        block_rows = math.gcd(row_count, 512)

        def absorb_block(block_index, running_state):
            key_part = lax.dynamic_slice_in_dim(key_block, block_index * block_rows, block_rows, 0)
            value_part = lax.dynamic_slice_in_dim(
                value_block, block_index * block_rows, block_rows, 0
            )
            return combine(
                running_state, fragment_contributions(queries, key_part, value_part, None)
            )

        return lax.fori_loop(0, row_count // block_rows, absorb_block, running)

    first_state = fragment_contributions(queries, text_k, text_v, text_valid)
    maxima, totals, accum = fold_inward(
        first_state,
        (
            lax.all_gather(k_local, "uly", axis=0, tiled=True),
            lax.all_gather(v_local, "uly", axis=0, tiled=True),
        ),
    )
    attended = jnp.transpose(accum / totals[..., None], (1, 0, 2)).astype(jnp.bfloat16)
    vid_out = lax.all_to_all(attended[:video_rows], "blk", split_axis=0, concat_axis=1, tiled=True)
    txt_out = attended[video_rows:]
    return (vid_out, txt_out)


def peer_id(flat, uly_count):
    return {"blk": flat // uly_count, "uly": flat % uly_count}


def lane_mask(shape, half):
    return lax.broadcasted_iota(jnp.int32, shape, len(shape) - 1) < half


def unit_rows(rows):
    return rows * lax.rsqrt(jnp.mean(rows * rows, axis=-1, keepdims=True) + EPSILON)


def fused_kernel(
    blk_count,
    uly_count,
    vq_hbm,
    vk_hbm,
    vv_hbm,
    tq_hbm,
    tk_hbm,
    tv_hbm,
    vq_gain,
    vk_gain,
    tq_gain,
    tk_gain,
    sharp,
    valid,
    vid_out,
    txt_out,
    vq_in,
    vk_in,
    vv_in,
    tq_in,
    tk_in,
    tv_in,
    kv_wide,
    q_wide,
    send,
    recv,
    text_kv,
    values,
    text_q,
    back_send,
    back_recv,
    back_wide,
    text_send,
    text_recv,
    in_sem,
    send_sem,
    recv_sem,
    back_send_sem,
    back_recv_sem,
    text_send_sem,
    text_recv_sem,
):
    count = blk_count * uly_count
    my_blk = lax.axis_index("blk")
    my_uly = lax.axis_index("uly")
    me = my_blk * uly_count + my_uly
    tokens, heads, width = vq_in.shape
    half_tokens = tokens // 2
    _, text_tokens = tq_in.shape
    text_share = text_tokens // uly_count
    lanes = 2 * width

    barrier = pltpu.get_barrier_semaphore()

    def greet(step, carry):
        peer = (me + 1 + step) % count
        pl.semaphore_signal(
            barrier, inc=1, device_id=peer_id(peer, uly_count), device_id_type=MESH
        )
        return carry

    lax.fori_loop(0, count - 1, greet, 0)

    loads = []
    for slot, (source, target) in enumerate(
        ((vk_hbm, vk_in), (vv_hbm, vv_in), (vq_hbm, vq_in))
    ):
        loads.append(pltpu.make_async_copy(source, target, in_sem.at[slot]))
    for slot, (source, target) in enumerate(
        ((tk_hbm, tk_in), (tv_hbm, tv_in), (tq_hbm, tq_in))
    ):
        loads.append(
            pltpu.make_async_copy(source.at[me], target, in_sem.at[3 + slot])
        )
    for load in loads:
        load.start()

    sharp_row = sharp[...] / math.sqrt(width)
    square = (heads, heads)
    sharp_column = jnp.sum(
        jnp.where(
            lax.broadcasted_iota(jnp.int32, square, 0) == lax.broadcasted_iota(jnp.int32, square, 1),
            jnp.broadcast_to(sharp_row, square),
            0.0,
        ),
        axis=1,
        keepdims=True,
    )
    my_sharp = jnp.sum(
        jnp.where(lax.broadcasted_iota(jnp.int32, (1, heads), 1) == me, sharp_row, 0.0),
        axis=1,
        keepdims=True,
    )

    loads[0].wait()
    loads[1].wait()
    keys = unit_rows(vk_in[...].astype(jnp.float32)) * vk_gain[...][None]
    kv_wide[...] = jnp.concatenate([keys, vv_in[...].astype(jnp.float32)], axis=-1)
    loads[2].wait()
    probes = unit_rows(vq_in[...].astype(jnp.float32)) * vq_gain[...][None] * sharp_column[None]
    q_wide[...] = jnp.concatenate([probes[:half_tokens], probes[half_tokens:]], axis=-1)
    for head in range(heads):
        send[head, :tokens, :] = kv_wide[:, head, :].astype(jnp.bfloat16)
        send[head, tokens:, :] = q_wide[:, head, :].astype(jnp.bfloat16)
    recv[me] = send[me]

    pl.semaphore_wait(barrier, count - 1)

    def outward(peer):
        return pltpu.make_async_remote_copy(
            src_ref=send.at[peer],
            dst_ref=recv.at[me],
            send_sem=send_sem.at[peer],
            recv_sem=recv_sem.at[me],
            device_id=peer_id(peer, uly_count),
            device_id_type=MESH,
        )

    def inward(peer):
        return pltpu.make_async_remote_copy(
            src_ref=send.at[peer],
            dst_ref=recv.at[peer],
            send_sem=send_sem.at[peer],
            recv_sem=recv_sem.at[peer],
            device_id=peer_id(peer, uly_count),
            device_id_type=MESH,
        )

    def dispatch(step, carry):
        distance = count // 2 + (1 - 2 * (step % 2)) * ((step + 1) // 2)
        outward((me + distance) % count).start()
        return carry

    lax.fori_loop(0, count - 1, dispatch, 0)

    def text_columns(text_in):
        return text_in[...].astype(jnp.float32).T

    loads[3].wait()
    loads[4].wait()
    both = jnp.concatenate(
        [unit_rows(text_columns(tk_in)) * tk_gain[...], text_columns(tv_in)], axis=-1
    )
    text_kv[...] = both.astype(jnp.bfloat16)
    video_tokens = count * tokens
    values[video_tokens:, :] = jnp.where(lane_mask(both.shape, width), 1.0, both).astype(
        jnp.bfloat16
    )
    loads[5].wait()
    text_probes = unit_rows(text_columns(tq_in)) * tq_gain[...] * my_sharp
    text_q[...] = jnp.concatenate([text_probes, jnp.zeros_like(text_probes)], axis=-1).astype(
        jnp.bfloat16
    )
    bias = jnp.where(valid[...] == 1, 0.0, NEGATIVE)

    def arrive(step, carry):
        inward((me + 1 + step) % count).wait_recv()
        return carry

    lax.fori_loop(0, count - 1, arrive, 0)

    video_kv = recv[:, :tokens, :].reshape(video_tokens, lanes)
    values[:video_tokens, :] = jnp.where(
        lane_mask(video_kv.shape, width), 1.0, video_kv.astype(jnp.float32)
    ).astype(jnp.bfloat16)

    def attend(rows):
        video_scores = lax.dot_general(
            rows,
            recv[:, :tokens, :].reshape(video_tokens, lanes),
            (((1,), (1,)), ((), ())),
            preferred_element_type=jnp.float32,
        )
        text_scores = (
            lax.dot_general(
                rows,
                text_kv[...],
                (((1,), (1,)), ((), ())),
                preferred_element_type=jnp.float32,
            )
            + bias
        )
        peak = jnp.maximum(
            jnp.max(video_scores, axis=1, keepdims=True),
            jnp.max(text_scores, axis=1, keepdims=True),
        )
        video_weights = jnp.exp(video_scores - peak).astype(jnp.bfloat16)
        text_weights = jnp.exp(text_scores - peak).astype(jnp.bfloat16)
        total = jnp.dot(
            video_weights, values[:video_tokens, :], preferred_element_type=jnp.float32
        ) + jnp.dot(text_weights, values[video_tokens:, :], preferred_element_type=jnp.float32)
        return total / pltpu.roll(total, width, 1)

    def pair_up(first, second):
        return jnp.where(lane_mask(first.shape, width), pltpu.roll(first, width, 1), second)

    def homeward(peer):
        return pltpu.make_async_remote_copy(
            src_ref=back_send.at[peer],
            dst_ref=back_recv.at[me],
            send_sem=back_send_sem.at[peer],
            recv_sem=back_recv_sem.at[me],
            device_id=peer_id(peer, uly_count),
            device_id_type=MESH,
        )

    def returned(peer):
        return pltpu.make_async_remote_copy(
            src_ref=back_send.at[peer],
            dst_ref=back_recv.at[peer],
            send_sem=back_send_sem.at[peer],
            recv_sem=back_recv_sem.at[peer],
            device_id=peer_id(peer, uly_count),
            device_id_type=MESH,
        )

    group = math.gcd(count, 8)
    group_count = count // group
    group_rows = group * half_tokens

    def video_group(step, carry):
        which = (me // group + group_count // 2 + step) % group_count
        first_peer = pl.multiple_of(which * group, group)
        packed = (
            recv[pl.ds(first_peer, group), tokens:, :]
            .reshape(group_rows, lanes)
            .astype(jnp.float32)
        )
        low = lane_mask(packed.shape, width)
        rows = jnp.concatenate(
            [jnp.where(low, packed, 0.0), jnp.where(low, pltpu.roll(packed, width, 1), 0.0)], axis=0
        ).astype(jnp.bfloat16)
        attended = attend(rows)
        back_send[pl.ds(first_peer, group)] = (
            pair_up(attended[:group_rows], attended[group_rows:])
            .astype(jnp.bfloat16)
            .reshape(group, half_tokens, lanes)
        )

        def hand_back(index, inner):
            peer = first_peer + (index + me) % group

            @pl.when(peer != me)
            def _():
                homeward(peer).start()

            return inner

        lax.fori_loop(0, group, hand_back, 0)
        return carry

    lax.fori_loop(0, group_count, video_group, 0)
    back_recv[me] = back_send[me]

    attended = attend(text_q[...])
    turned = attended.T[width:]
    for part in range(uly_count):
        text_send[part] = turned[:, part * text_share : (part + 1) * text_share].astype(
            jnp.bfloat16
        )

    def text_copy(part, slot):
        return pltpu.make_async_remote_copy(
            src_ref=text_send.at[part],
            dst_ref=text_recv.at[slot],
            send_sem=text_send_sem.at[part],
            recv_sem=text_recv_sem.at[slot],
            device_id={"blk": my_blk, "uly": part},
            device_id_type=MESH,
        )

    for step in range(1, uly_count):
        text_copy((my_uly + step) % uly_count, my_uly).start()
    text_recv[my_uly] = text_send[my_uly]

    for step in range(1, uly_count):
        other = (my_uly + step) % uly_count
        text_copy(other, other).wait_recv()
    txt_out[...] = text_recv[...]

    def collect(step, carry):
        returned((me + 1 + step) % count).wait_recv()
        return carry

    lax.fori_loop(0, count - 1, collect, 0)
    for head in range(heads):
        back_wide[:, head, :] = back_recv[head].astype(jnp.float32)
    vid_out[:half_tokens] = back_wide[:, :, :width].astype(jnp.bfloat16)
    vid_out[half_tokens:] = back_wide[:, :, width:].astype(jnp.bfloat16)

    def drain(step, carry):
        peer = (me + 1 + step) % count
        outward(peer).wait_send()
        homeward(peer).wait_send()
        return carry

    lax.fori_loop(0, count - 1, drain, 0)
    for step in range(1, uly_count):
        text_copy((my_uly + step) % uly_count, my_uly).wait_send()


def fused_on_device(blk_count, uly_count, *operands):
    vq, vk, vv, tq, tk, tv, vq_gain, vk_gain, tq_gain, tk_gain, sharp, valid = operands
    tokens, heads, width = vq.shape
    text_tokens = tq.shape[0]
    count = blk_count * uly_count
    lanes = 2 * width
    text_share = text_tokens // uly_count
    half = tokens // 2
    bf16, f32 = jnp.bfloat16, jnp.float32
    any_spec = pl.BlockSpec(memory_space=pl.ANY)
    vmem_spec = pl.BlockSpec(memory_space=pltpu.VMEM)
    dma = pltpu.SemaphoreType.DMA
    vid_out, txt_out = pl.pallas_call(
        functools.partial(fused_kernel, blk_count, uly_count),
        out_shape=(
            jax.ShapeDtypeStruct((tokens, heads, width), bf16),
            jax.ShapeDtypeStruct((uly_count, width, text_share), bf16),
        ),
        in_specs=[any_spec] * 6 + [vmem_spec] * 6,
        out_specs=(vmem_spec, vmem_spec),
        scratch_shapes=[
            pltpu.VMEM((tokens, heads, width), bf16),
            pltpu.VMEM((tokens, heads, width), bf16),
            pltpu.VMEM((tokens, heads, width), bf16),
            pltpu.VMEM((width, text_tokens), bf16),
            pltpu.VMEM((width, text_tokens), bf16),
            pltpu.VMEM((width, text_tokens), bf16),
            pltpu.VMEM((tokens, heads, lanes), f32),
            pltpu.VMEM((half, heads, lanes), f32),
            pltpu.VMEM((count, tokens + half, lanes), bf16),
            pltpu.VMEM((count, tokens + half, lanes), bf16),
            pltpu.VMEM((text_tokens, lanes), bf16),
            pltpu.VMEM((count * tokens + text_tokens, lanes), bf16),
            pltpu.VMEM((text_tokens, lanes), bf16),
            pltpu.VMEM((count, half, lanes), bf16),
            pltpu.VMEM((count, half, lanes), bf16),
            pltpu.VMEM((half, heads, lanes), f32),
            pltpu.VMEM((uly_count, width, text_share), bf16),
            pltpu.VMEM((uly_count, width, text_share), bf16),
            dma((6,)),
            dma((count,)),
            dma((count,)),
            dma((count,)),
            dma((count,)),
            dma((uly_count,)),
            dma((uly_count,)),
        ],
        compiler_params=pltpu.CompilerParams(collective_id=0, has_side_effects=True),
        name="joint_attention",
    )(
        vq,
        vk,
        vv,
        jnp.transpose(tq, (1, 2, 0)),
        jnp.transpose(tk, (1, 2, 0)),
        jnp.transpose(tv, (1, 2, 0)),
        vq_gain[None],
        vk_gain[None],
        tq_gain[None],
        tk_gain[None],
        sharp[None],
        valid[None],
    )
    return vid_out, jnp.transpose(txt_out, (2, 0, 1))


def fits_fused(mesh, vq, tq):
    count = mesh.shape["blk"] * mesh.shape["uly"]
    tokens = vq.shape[0] // count
    return (
        vq.shape[1] == count
        and 2 * vq.shape[2] == 128
        and tokens % 32 == 0
        and tokens <= 64
        and tq.shape[0] % (128 * mesh.shape["uly"]) == 0
    )


def solution(mesh):
    blk_count, uly_count = mesh.shape["blk"], mesh.shape["uly"]

    def run(*operands):
        body = on_device
        if fits_fused(mesh, operands[0], operands[3]):
            body = functools.partial(fused_on_device, blk_count, uly_count)
        split = P(("blk", "uly"), None, None)
        return jax.shard_map(
            body,
            mesh=mesh,
            in_specs=(split, split, split) + (P(),) * 9,
            out_specs=(split, P("uly", "blk", None)),
            check_vma=False,
        )(*operands)

    return run
```

```python
import functools
import math

import jax
import jax.numpy as jnp
from jax import lax
from jax.experimental import pallas as pl
from jax.experimental.pallas import tpu as pltpu
from jax.sharding import PartitionSpec as P

EPSILON = 1e-06
NEGATIVE = -1e30
MESH = pl.DeviceIdType.MESH


def normed(tensor, gain_vector, rescale_factor):
    widened = tensor.astype(jnp.float32)
    inverse = lax.rsqrt(jnp.mean(widened * widened, axis=-1, keepdims=True) + EPSILON)
    return (widened * inverse * gain_vector * rescale_factor).astype(jnp.bfloat16)


def fragment_contributions(queries, key_rows, value_rows, valid):
    scores = jnp.einsum("qhd,khd->hqk", queries, key_rows, preferred_element_type=jnp.float32)
    if valid is not None:
        scores = jnp.where(valid[None, None, :], scores, NEGATIVE)
    maxima = jnp.max(scores, axis=-1)
    weights = jnp.exp(scores - maxima[..., None])
    if valid is not None:
        weights = jnp.where(valid[None, None, :], weights, 0.0)
    totals = jnp.sum(weights, axis=-1)
    accum = jnp.einsum(
        "hqk,khd->hqd", weights, value_rows.astype(jnp.float32), precision=lax.Precision.HIGHEST
    )
    return (maxima, totals, accum)


def combine(earlier, later):
    max_one, total_one, accum_one = earlier
    max_two, total_two, accum_two = later
    merged_max = jnp.maximum(max_one, max_two)
    factor_one = jnp.exp(max_one - merged_max)
    factor_two = jnp.exp(max_two - merged_max)
    merged_total = total_one * factor_one + total_two * factor_two
    merged_accum = accum_one * factor_one[..., None] + accum_two * factor_two[..., None]
    return (merged_max, merged_total, merged_accum)


def on_device(
    footage_probes,
    footage_lookup_keys,
    footage_payload,
    caption_probes,
    caption_lookup_keys,
    caption_payload,
    footage_probes_amplitude,
    footage_keys_amplitude,
    caption_probes_amplitude,
    caption_keys_amplitude,
    focus_sharpness,
    caption_validity,
):
    channel_width = footage_probes.shape[2]
    rescale_factor = focus_sharpness[None, :, None] / math.sqrt(channel_width)
    q_norm = normed(footage_probes, footage_probes_amplitude, rescale_factor)
    k_norm = normed(footage_lookup_keys, footage_keys_amplitude, 1.0)
    q_local = lax.all_to_all(q_norm, "blk", split_axis=1, concat_axis=0, tiled=True)
    k_local = lax.all_to_all(k_norm, "blk", split_axis=1, concat_axis=0, tiled=True)
    v_local = lax.all_to_all(footage_payload, "blk", split_axis=1, concat_axis=0, tiled=True)
    local_heads = q_local.shape[1]
    head_start = lax.axis_index("blk") * local_heads
    local_scale = lax.dynamic_slice_in_dim(rescale_factor, head_start, local_heads, 1)
    text_q = normed(
        lax.dynamic_slice_in_dim(caption_probes, head_start, local_heads, 1),
        caption_probes_amplitude,
        local_scale,
    )
    text_k = normed(
        lax.dynamic_slice_in_dim(caption_lookup_keys, head_start, local_heads, 1),
        caption_keys_amplitude,
        1.0,
    )
    text_v = lax.dynamic_slice_in_dim(caption_payload, head_start, local_heads, 1)
    text_valid = caption_validity == 1
    text_share = caption_probes.shape[0] // lax.axis_size("uly")
    row_start = lax.axis_index("uly") * text_share
    video_rows = q_local.shape[0]
    queries = jnp.concatenate(
        [q_local, lax.dynamic_slice_in_dim(text_q, row_start, text_share, 0)], 0
    )

    def fold_inward(running, gathered):
        key_block, value_block = gathered
        row_count = key_block.shape[0]
        block_rows = math.gcd(row_count, 512)

        def absorb_block(block_index, running_state):
            key_part = lax.dynamic_slice_in_dim(key_block, block_index * block_rows, block_rows, 0)
            value_part = lax.dynamic_slice_in_dim(
                value_block, block_index * block_rows, block_rows, 0
            )
            return combine(
                running_state, fragment_contributions(queries, key_part, value_part, None)
            )

        return lax.fori_loop(0, row_count // block_rows, absorb_block, running)

    first_state = fragment_contributions(queries, text_k, text_v, text_valid)
    maxima, totals, accum = fold_inward(
        first_state,
        (
            lax.all_gather(k_local, "uly", axis=0, tiled=True),
            lax.all_gather(v_local, "uly", axis=0, tiled=True),
        ),
    )
    attended = jnp.transpose(accum / totals[..., None], (1, 0, 2)).astype(jnp.bfloat16)
    vid_out = lax.all_to_all(attended[:video_rows], "blk", split_axis=0, concat_axis=1, tiled=True)
    txt_out = attended[video_rows:]
    return (vid_out, txt_out)


def peer_id(flat, uly_count):
    return {"blk": flat // uly_count, "uly": flat % uly_count}


def lane_mask(shape, half):
    return lax.broadcasted_iota(jnp.int32, shape, len(shape) - 1) < half


def unit_rows(rows):
    return rows * lax.rsqrt(jnp.mean(rows * rows, axis=-1, keepdims=True) + EPSILON)


def fused_kernel(
    blk_count,
    uly_count,
    vq_hbm,
    vk_hbm,
    vv_hbm,
    tq_hbm,
    tk_hbm,
    tv_hbm,
    vq_gain,
    vk_gain,
    tq_gain,
    tk_gain,
    sharp,
    valid,
    back_out,
    txt_out,
    vq_in,
    vk_in,
    vv_in,
    tq_in,
    tk_in,
    tv_in,
    kv_wide,
    q_wide,
    send,
    recv,
    text_kv,
    queries,
    totals,
    peaks,
    back_send,
    back_recv,
    text_send,
    text_recv,
    in_sem,
    q_send_sem,
    q_recv_sem,
    send_sem,
    recv_sem,
    back_send_sem,
    back_recv_sem,
    text_send_sem,
    text_recv_sem,
):
    count = blk_count * uly_count
    my_blk = lax.axis_index("blk")
    my_uly = lax.axis_index("uly")
    me = my_blk * uly_count + my_uly
    tokens, heads, width = vq_in.shape
    half_tokens = tokens // 2
    _, text_tokens = tq_in.shape
    text_share = text_tokens // uly_count
    lanes = 2 * width

    barrier = pltpu.get_barrier_semaphore()

    def greet(step, carry):
        peer = (me + 1 + step) % count
        pl.semaphore_signal(
            barrier, inc=1, device_id=peer_id(peer, uly_count), device_id_type=MESH
        )
        return carry

    lax.fori_loop(0, count - 1, greet, 0)

    loads = []
    for slot, (source, target) in enumerate(
        ((vk_hbm, vk_in), (vv_hbm, vv_in), (vq_hbm, vq_in))
    ):
        loads.append(pltpu.make_async_copy(source, target, in_sem.at[slot]))
    for slot, (source, target) in enumerate(
        ((tk_hbm, tk_in), (tv_hbm, tv_in), (tq_hbm, tq_in))
    ):
        loads.append(
            pltpu.make_async_copy(source.at[me], target, in_sem.at[3 + slot])
        )
    for load in loads:
        load.start()

    sharp_row = sharp[...] / math.sqrt(width)
    square = (heads, heads)
    sharp_column = jnp.sum(
        jnp.where(
            lax.broadcasted_iota(jnp.int32, square, 0) == lax.broadcasted_iota(jnp.int32, square, 1),
            jnp.broadcast_to(sharp_row, square),
            0.0,
        ),
        axis=1,
        keepdims=True,
    )
    my_sharp = jnp.sum(
        jnp.where(lax.broadcasted_iota(jnp.int32, (1, heads), 1) == me, sharp_row, 0.0),
        axis=1,
        keepdims=True,
    )

    loads[0].wait()
    loads[1].wait()
    keys = unit_rows(vk_in[...].astype(jnp.float32)) * vk_gain[...][None]
    kv_wide[...] = jnp.concatenate([keys, vv_in[...].astype(jnp.float32)], axis=-1)
    loads[2].wait()
    probes = unit_rows(vq_in[...].astype(jnp.float32)) * vq_gain[...][None] * sharp_column[None]
    q_wide[...] = jnp.concatenate([probes[:half_tokens], probes[half_tokens:]], axis=-1)
    for head in range(heads):
        send[head, :tokens, :] = kv_wide[:, head, :].astype(jnp.bfloat16)
        send[head, tokens:, :] = q_wide[:, head, :].astype(jnp.bfloat16)
    recv[me] = send[me]

    pl.semaphore_wait(barrier, count - 1)

    query_part, kv_part = pl.ds(tokens, half_tokens), pl.ds(0, tokens)

    def outward(peer, part, sent, landed):
        return pltpu.make_async_remote_copy(
            src_ref=send.at[peer, part],
            dst_ref=recv.at[me, part],
            send_sem=sent.at[peer],
            recv_sem=landed.at[me],
            device_id=peer_id(peer, uly_count),
            device_id_type=MESH,
        )

    def inward(peer, part, sent, landed):
        return pltpu.make_async_remote_copy(
            src_ref=send.at[peer, part],
            dst_ref=recv.at[peer, part],
            send_sem=sent.at[peer],
            recv_sem=landed.at[peer],
            device_id=peer_id(peer, uly_count),
            device_id_type=MESH,
        )

    def dispatch_queries(step, carry):
        distance = count // 2 + (1 - 2 * (step % 2)) * ((step + 1) // 2)
        outward((me + distance) % count, query_part, q_send_sem, q_recv_sem).start()
        return carry

    lax.fori_loop(0, count - 1, dispatch_queries, 0)

    group = math.gcd(count, 8)
    group_count = count // group
    my_group = me // group
    if group_count == 4:
        near = my_group + 1 - 2 * (my_group % 2)
        planes = [my_group, near, (my_group + 2) % 4, 3 - my_group]
    else:
        planes = [(my_group + step) % group_count for step in range(group_count)]

    for plane in planes:

        def dispatch(step, carry, plane=plane):
            peer = plane * group + (step + me) % group

            @pl.when(peer != me)
            def _():
                outward(peer, kv_part, send_sem, recv_sem).start()

            return carry

        lax.fori_loop(0, group, dispatch, 0)

    def text_columns(text_in):
        return text_in[...].astype(jnp.float32).T

    loads[3].wait()
    loads[4].wait()
    both = jnp.concatenate(
        [unit_rows(text_columns(tk_in)) * tk_gain[...], text_columns(tv_in)], axis=-1
    )
    text_kv[...] = both.astype(jnp.bfloat16)
    loads[5].wait()
    text_probes = unit_rows(text_columns(tq_in)) * tq_gain[...] * my_sharp
    block = group * tokens
    queries[count * tokens :, :] = jnp.concatenate([text_probes, jnp.zeros_like(text_probes)], axis=-1).astype(
        jnp.bfloat16
    )
    bias = jnp.where(valid[...] == 1, 0.0, NEGATIVE)

    def with_ones(pairs):
        return jnp.where(lane_mask(pairs.shape, width), 1.0, pairs.astype(jnp.float32)).astype(
            jnp.bfloat16
        )

    def scores_of(rows, pairs):
        return lax.dot_general(
            rows, pairs, (((1,), (1,)), ((), ())), preferred_element_type=jnp.float32
        )

    def row_max(scores):
        return jnp.max(scores, axis=1, keepdims=True)

    def weighted(scores, peak, pairs):
        return jnp.dot(
            jnp.exp(scores - peak).astype(jnp.bfloat16), pairs, preferred_element_type=jnp.float32
        )

    def arrive_queries(step, carry):
        inward((me + 1 + step) % count, query_part, q_send_sem, q_recv_sem).wait_recv()
        return carry

    lax.fori_loop(0, count - 1, arrive_queries, 0)
    group_rows = group * half_tokens
    for index in range(group_count):
        packed = (
            recv[index * group : (index + 1) * group, tokens:, :]
            .reshape(group_rows, lanes)
            .astype(jnp.float32)
        )
        low = lane_mask(packed.shape, width)
        for side, rows in enumerate((packed, pltpu.roll(packed, width, 1))):
            start = index * block + side * group_rows
            queries[start : start + group_rows, :] = jnp.where(low, rows, 0.0).astype(jnp.bfloat16)

    def plane_pairs(plane):
        def arrive(step, carry):
            peer = plane * group + step

            @pl.when(peer != me)
            def _():
                inward(peer, kv_part, send_sem, recv_sem).wait_recv()

            return carry

        lax.fori_loop(0, group, arrive, 0)
        first = pl.multiple_of(plane * group, group)
        return recv[pl.ds(first, group), :tokens, :].reshape(block, lanes)

    block_count = group_count + text_tokens // block

    def block_rows(index):
        return pl.ds(pl.multiple_of(index * block, block), block)

    text_ones = with_ones(text_kv[...])
    pairs = plane_pairs(planes[0])
    ones = with_ones(pairs)
    for index in range(block_count):
        rows = queries[block_rows(index), :]
        scores = scores_of(rows, pairs)
        text_scores = scores_of(rows, text_kv[...]) + bias
        peak = jnp.maximum(row_max(scores), row_max(text_scores))
        totals[block_rows(index), :] = weighted(scores, peak, ones) + weighted(
            text_scores, peak, text_ones
        )
        peaks[block_rows(index), :] = peak

    def absorb(index, pairs, ones):
        scores = scores_of(queries[block_rows(index), :], pairs)
        earlier = peaks[block_rows(index), :]
        peak = jnp.maximum(earlier, row_max(scores))
        total = totals[block_rows(index), :] * jnp.exp(earlier - peak) + weighted(
            scores, peak, ones
        )
        return peak, total

    for plane in planes[1:-1]:
        pairs = plane_pairs(plane)
        ones = with_ones(pairs)
        for index in range(block_count):
            peak, total = absorb(index, pairs, ones)
            totals[block_rows(index), :] = total
            peaks[block_rows(index), :] = peak

    pairs = plane_pairs(planes[-1])
    ones = with_ones(pairs)

    def attend(index):
        _, total = absorb(index, pairs, ones)
        return total / pltpu.roll(total, width, 1)

    def pair_up(first, second):
        return jnp.where(lane_mask(first.shape, width), pltpu.roll(first, width, 1), second)

    def homeward(peer):
        return pltpu.make_async_remote_copy(
            src_ref=back_send.at[peer],
            dst_ref=back_recv.at[me],
            send_sem=back_send_sem.at[peer],
            recv_sem=back_recv_sem.at[me],
            device_id=peer_id(peer, uly_count),
            device_id_type=MESH,
        )

    def returned(peer):
        return pltpu.make_async_remote_copy(
            src_ref=back_send.at[peer],
            dst_ref=back_recv.at[peer],
            send_sem=back_send_sem.at[peer],
            recv_sem=back_recv_sem.at[peer],
            device_id=peer_id(peer, uly_count),
            device_id_type=MESH,
        )

    for which in planes[::-1]:
        first_peer = pl.multiple_of(which * group, group)
        attended = attend(which)
        back_send[pl.ds(first_peer, group)] = (
            pair_up(attended[:group_rows], attended[group_rows:])
            .astype(jnp.bfloat16)
            .reshape(group, half_tokens, lanes)
        )

        def hand_back(step, carry, first_peer=first_peer):
            peer = first_peer + (step + me) % group

            @pl.when(peer != me)
            def _():
                homeward(peer).start()

            return carry

        lax.fori_loop(0, group, hand_back, 0)
    back_recv[me] = back_send[me]

    attended = jnp.concatenate(
        [attend(index) for index in range(group_count, block_count)], axis=0
    )
    turned = attended.T[width:]
    for part in range(uly_count):
        text_send[part] = turned[:, part * text_share : (part + 1) * text_share].astype(
            jnp.bfloat16
        )

    def text_copy(part, slot):
        return pltpu.make_async_remote_copy(
            src_ref=text_send.at[part],
            dst_ref=text_recv.at[slot],
            send_sem=text_send_sem.at[part],
            recv_sem=text_recv_sem.at[slot],
            device_id={"blk": my_blk, "uly": part},
            device_id_type=MESH,
        )

    for step in range(1, uly_count):
        text_copy((my_uly + step) % uly_count, my_uly).start()
    text_recv[my_uly] = text_send[my_uly]

    for step in range(1, uly_count):
        other = (my_uly + step) % uly_count
        text_copy(other, other).wait_recv()
    txt_out[...] = text_recv[...]

    def collect(step, carry):
        returned((me + 1 + step) % count).wait_recv()
        return carry

    lax.fori_loop(0, count - 1, collect, 0)
    back_out[...] = back_recv[...]

    def drain(step, carry):
        peer = (me + 1 + step) % count
        outward(peer, query_part, q_send_sem, q_recv_sem).wait_send()
        outward(peer, kv_part, send_sem, recv_sem).wait_send()
        homeward(peer).wait_send()
        return carry

    lax.fori_loop(0, count - 1, drain, 0)
    for step in range(1, uly_count):
        text_copy((my_uly + step) % uly_count, my_uly).wait_send()


def lay_out_kernel(back_ref, txt_ref, vid_out, txt_out, wide):
    heads, half, lanes = back_ref.shape
    width = lanes // 2
    for head in range(heads):
        wide[:, head, :] = back_ref[head].astype(jnp.float32)
    vid_out[:half] = wide[:, :, :width].astype(jnp.bfloat16)
    vid_out[half:] = wide[:, :, width:].astype(jnp.bfloat16)
    txt_out[...] = txt_ref[...]


def fused_on_device(blk_count, uly_count, *operands):
    vq, vk, vv, tq, tk, tv, vq_gain, vk_gain, tq_gain, tk_gain, sharp, valid = operands
    tokens, heads, width = vq.shape
    text_tokens = tq.shape[0]
    count = blk_count * uly_count
    lanes = 2 * width
    text_share = text_tokens // uly_count
    half = tokens // 2
    bf16, f32 = jnp.bfloat16, jnp.float32
    any_spec = pl.BlockSpec(memory_space=pl.ANY)
    vmem_spec = pl.BlockSpec(memory_space=pltpu.VMEM)
    dma = pltpu.SemaphoreType.DMA
    text_shape = jax.ShapeDtypeStruct((uly_count, width, text_share), bf16)
    back, text_back = pl.pallas_call(
        functools.partial(fused_kernel, blk_count, uly_count),
        out_shape=(
            jax.ShapeDtypeStruct((count, half, lanes), bf16),
            text_shape,
        ),
        in_specs=[any_spec] * 6 + [vmem_spec] * 6,
        out_specs=(vmem_spec, vmem_spec),
        scratch_shapes=[
            pltpu.VMEM((tokens, heads, width), bf16),
            pltpu.VMEM((tokens, heads, width), bf16),
            pltpu.VMEM((tokens, heads, width), bf16),
            pltpu.VMEM((width, text_tokens), bf16),
            pltpu.VMEM((width, text_tokens), bf16),
            pltpu.VMEM((width, text_tokens), bf16),
            pltpu.VMEM((tokens, heads, lanes), f32),
            pltpu.VMEM((half, heads, lanes), f32),
            pltpu.VMEM((count, tokens + half, lanes), bf16),
            pltpu.VMEM((count, tokens + half, lanes), bf16),
            pltpu.VMEM((text_tokens, lanes), bf16),
            pltpu.VMEM((count * tokens + text_tokens, lanes), bf16),
            pltpu.VMEM((count * tokens + text_tokens, lanes), f32),
            pltpu.VMEM((count * tokens + text_tokens, 1), f32),
            pltpu.VMEM((count, half, lanes), bf16),
            pltpu.VMEM((count, half, lanes), bf16),
            pltpu.VMEM((uly_count, width, text_share), bf16),
            pltpu.VMEM((uly_count, width, text_share), bf16),
            dma((6,)),
            dma((count,)),
            dma((count,)),
            dma((count,)),
            dma((count,)),
            dma((count,)),
            dma((count,)),
            dma((uly_count,)),
            dma((uly_count,)),
        ],
        compiler_params=pltpu.CompilerParams(collective_id=0, has_side_effects=True),
        name="joint_attention",
    )(
        vq,
        vk,
        vv,
        jnp.transpose(tq, (1, 2, 0)),
        jnp.transpose(tk, (1, 2, 0)),
        jnp.transpose(tv, (1, 2, 0)),
        vq_gain[None],
        vk_gain[None],
        tq_gain[None],
        tk_gain[None],
        sharp[None],
        valid[None],
    )
    vid_out, txt_out = pl.pallas_call(
        lay_out_kernel,
        out_shape=(jax.ShapeDtypeStruct((tokens, heads, width), bf16), text_shape),
        in_specs=[vmem_spec] * 2,
        out_specs=(vmem_spec, vmem_spec),
        scratch_shapes=[pltpu.VMEM((half, heads, lanes), f32)],
        name="lay_out",
    )(back, text_back)
    return vid_out, jnp.transpose(txt_out, (2, 0, 1))


def fits_fused(mesh, vq, tq):
    count = mesh.shape["blk"] * mesh.shape["uly"]
    tokens = vq.shape[0] // count
    return (
        vq.shape[1] == count
        and 2 * vq.shape[2] == 128
        and tokens % 32 == 0
        and tokens <= 64
        and tq.shape[0] % (math.gcd(count, 8) * tokens) == 0
        and tq.shape[0] % (128 * mesh.shape["uly"]) == 0
    )


def solution(mesh):
    blk_count, uly_count = mesh.shape["blk"], mesh.shape["uly"]

    def run(*operands):
        body = on_device
        if fits_fused(mesh, operands[0], operands[3]):
            body = functools.partial(fused_on_device, blk_count, uly_count)
        split = P(("blk", "uly"), None, None)
        return jax.shard_map(
            body,
            mesh=mesh,
            in_specs=(split, split, split) + (P(),) * 9,
            out_specs=(split, P("uly", "blk", None)),
            check_vma=False,
        )(*operands)

    return run
```

```python
import functools
import math

import jax
import jax.numpy as jnp
from jax import lax
from jax.experimental import pallas as pl
from jax.experimental.pallas import tpu as pltpu
from jax.sharding import PartitionSpec as P

EPSILON = 1e-06
NEGATIVE = -1e30
MESH = pl.DeviceIdType.MESH


def normed(tensor, gain_vector, rescale_factor):
    widened = tensor.astype(jnp.float32)
    inverse = lax.rsqrt(jnp.mean(widened * widened, axis=-1, keepdims=True) + EPSILON)
    return (widened * inverse * gain_vector * rescale_factor).astype(jnp.bfloat16)


def fragment_contributions(queries, key_rows, value_rows, valid):
    scores = jnp.einsum("qhd,khd->hqk", queries, key_rows, preferred_element_type=jnp.float32)
    if valid is not None:
        scores = jnp.where(valid[None, None, :], scores, NEGATIVE)
    maxima = jnp.max(scores, axis=-1)
    weights = jnp.exp(scores - maxima[..., None])
    if valid is not None:
        weights = jnp.where(valid[None, None, :], weights, 0.0)
    totals = jnp.sum(weights, axis=-1)
    accum = jnp.einsum(
        "hqk,khd->hqd", weights, value_rows.astype(jnp.float32), precision=lax.Precision.HIGHEST
    )
    return (maxima, totals, accum)


def combine(earlier, later):
    max_one, total_one, accum_one = earlier
    max_two, total_two, accum_two = later
    merged_max = jnp.maximum(max_one, max_two)
    factor_one = jnp.exp(max_one - merged_max)
    factor_two = jnp.exp(max_two - merged_max)
    merged_total = total_one * factor_one + total_two * factor_two
    merged_accum = accum_one * factor_one[..., None] + accum_two * factor_two[..., None]
    return (merged_max, merged_total, merged_accum)


def on_device(
    footage_probes,
    footage_lookup_keys,
    footage_payload,
    caption_probes,
    caption_lookup_keys,
    caption_payload,
    footage_probes_amplitude,
    footage_keys_amplitude,
    caption_probes_amplitude,
    caption_keys_amplitude,
    focus_sharpness,
    caption_validity,
):
    channel_width = footage_probes.shape[2]
    rescale_factor = focus_sharpness[None, :, None] / math.sqrt(channel_width)
    q_norm = normed(footage_probes, footage_probes_amplitude, rescale_factor)
    k_norm = normed(footage_lookup_keys, footage_keys_amplitude, 1.0)
    q_local = lax.all_to_all(q_norm, "blk", split_axis=1, concat_axis=0, tiled=True)
    k_local = lax.all_to_all(k_norm, "blk", split_axis=1, concat_axis=0, tiled=True)
    v_local = lax.all_to_all(footage_payload, "blk", split_axis=1, concat_axis=0, tiled=True)
    local_heads = q_local.shape[1]
    head_start = lax.axis_index("blk") * local_heads
    local_scale = lax.dynamic_slice_in_dim(rescale_factor, head_start, local_heads, 1)
    text_q = normed(
        lax.dynamic_slice_in_dim(caption_probes, head_start, local_heads, 1),
        caption_probes_amplitude,
        local_scale,
    )
    text_k = normed(
        lax.dynamic_slice_in_dim(caption_lookup_keys, head_start, local_heads, 1),
        caption_keys_amplitude,
        1.0,
    )
    text_v = lax.dynamic_slice_in_dim(caption_payload, head_start, local_heads, 1)
    text_valid = caption_validity == 1
    text_share = caption_probes.shape[0] // lax.axis_size("uly")
    row_start = lax.axis_index("uly") * text_share
    video_rows = q_local.shape[0]
    queries = jnp.concatenate(
        [q_local, lax.dynamic_slice_in_dim(text_q, row_start, text_share, 0)], 0
    )

    def fold_inward(running, gathered):
        key_block, value_block = gathered
        row_count = key_block.shape[0]
        block_rows = math.gcd(row_count, 512)

        def absorb_block(block_index, running_state):
            key_part = lax.dynamic_slice_in_dim(key_block, block_index * block_rows, block_rows, 0)
            value_part = lax.dynamic_slice_in_dim(
                value_block, block_index * block_rows, block_rows, 0
            )
            return combine(
                running_state, fragment_contributions(queries, key_part, value_part, None)
            )

        return lax.fori_loop(0, row_count // block_rows, absorb_block, running)

    first_state = fragment_contributions(queries, text_k, text_v, text_valid)
    maxima, totals, accum = fold_inward(
        first_state,
        (
            lax.all_gather(k_local, "uly", axis=0, tiled=True),
            lax.all_gather(v_local, "uly", axis=0, tiled=True),
        ),
    )
    attended = jnp.transpose(accum / totals[..., None], (1, 0, 2)).astype(jnp.bfloat16)
    vid_out = lax.all_to_all(attended[:video_rows], "blk", split_axis=0, concat_axis=1, tiled=True)
    txt_out = attended[video_rows:]
    return (vid_out, txt_out)


def peer_id(flat, uly_count):
    return {"blk": flat // uly_count, "uly": flat % uly_count}


def lane_mask(shape, half):
    return lax.broadcasted_iota(jnp.int32, shape, len(shape) - 1) < half


def unit_rows(rows):
    return rows * lax.rsqrt(jnp.mean(rows * rows, axis=-1, keepdims=True) + EPSILON)


def fused_kernel(
    blk_count,
    uly_count,
    vq_hbm,
    vk_hbm,
    vv_hbm,
    tq_hbm,
    tk_hbm,
    tv_hbm,
    vq_gain_hbm,
    vk_gain_hbm,
    tq_gain_hbm,
    tk_gain_hbm,
    sharp_hbm,
    valid_hbm,
    back_out,
    txt_out,
    vq_in,
    vk_in,
    vv_in,
    tq_in,
    tk_in,
    tv_in,
    vq_gain,
    vk_gain,
    tq_gain,
    tk_gain,
    sharp,
    valid,
    kv_wide,
    q_wide,
    send,
    recv,
    text_kv,
    queries,
    totals,
    peaks,
    back_send,
    text_send,
    in_sem,
    own_sem,
    q_send_sem,
    q_recv_sem,
    send_sem,
    recv_sem,
    back_send_sem,
    back_recv_sem,
    text_send_sem,
    text_recv_sem,
):
    count = blk_count * uly_count
    my_blk = lax.axis_index("blk")
    my_uly = lax.axis_index("uly")
    me = my_blk * uly_count + my_uly
    tokens, heads, width = vq_in.shape
    half_tokens = tokens // 2
    _, text_tokens = tq_in.shape
    text_share = text_tokens // uly_count
    lanes = 2 * width

    barrier = pltpu.get_barrier_semaphore()

    def greet(step, carry):
        distance = count // 2 + (1 - 2 * (step % 2)) * ((step + 1) // 2)
        peer = (me + distance) % count
        pl.semaphore_signal(
            barrier, inc=1, device_id=peer_id(peer, uly_count), device_id_type=MESH
        )
        return carry

    lax.fori_loop(0, count - 1, greet, 0)

    loads = []
    for slot, (source, target) in enumerate(
        ((vk_hbm, vk_in), (vv_hbm, vv_in), (vq_hbm, vq_in))
    ):
        loads.append(pltpu.make_async_copy(source, target, in_sem.at[slot]))
    for slot, (source, target) in enumerate(
        ((tk_hbm, tk_in), (tv_hbm, tv_in), (tq_hbm, tq_in))
    ):
        loads.append(
            pltpu.make_async_copy(source.at[me], target, in_sem.at[3 + slot])
        )
    small = []
    for slot, (source, target) in enumerate(
        (
            (vk_gain_hbm, vk_gain),
            (vq_gain_hbm, vq_gain),
            (sharp_hbm, sharp),
            (tk_gain_hbm, tk_gain),
            (tq_gain_hbm, tq_gain),
            (valid_hbm, valid),
        )
    ):
        small.append(pltpu.make_async_copy(source, target, in_sem.at[6 + slot]))
    for load in small + loads:
        load.start()
    for load in small:
        load.wait()

    sharp_row = sharp[...] / math.sqrt(width)
    square = (heads, heads)
    sharp_column = jnp.sum(
        jnp.where(
            lax.broadcasted_iota(jnp.int32, square, 0) == lax.broadcasted_iota(jnp.int32, square, 1),
            jnp.broadcast_to(sharp_row, square),
            0.0,
        ),
        axis=1,
        keepdims=True,
    )
    my_sharp = jnp.sum(
        jnp.where(lax.broadcasted_iota(jnp.int32, (1, heads), 1) == me, sharp_row, 0.0),
        axis=1,
        keepdims=True,
    )

    loads[0].wait()
    loads[1].wait()
    keys = unit_rows(vk_in[...].astype(jnp.float32)) * vk_gain[...][None]
    kv_wide[...] = jnp.concatenate([keys, vv_in[...].astype(jnp.float32)], axis=-1)
    loads[2].wait()
    probes = unit_rows(vq_in[...].astype(jnp.float32)) * vq_gain[...][None] * sharp_column[None]
    q_wide[...] = jnp.concatenate([probes[:half_tokens], probes[half_tokens:]], axis=-1)
    for head in range(heads):
        send[head, :tokens, :] = kv_wide[:, head, :].astype(jnp.bfloat16)
        send[head, tokens:, :] = q_wide[:, head, :].astype(jnp.bfloat16)
    recv[me] = send[me]

    pl.semaphore_wait(barrier, count - 1)

    query_part, kv_part = pl.ds(tokens, half_tokens), pl.ds(0, tokens)

    def outward(peer, part, sent, landed):
        return pltpu.make_async_remote_copy(
            src_ref=send.at[peer, part],
            dst_ref=recv.at[me, part],
            send_sem=sent.at[peer],
            recv_sem=landed.at[me],
            device_id=peer_id(peer, uly_count),
            device_id_type=MESH,
        )

    def inward(peer, part, sent, landed):
        return pltpu.make_async_remote_copy(
            src_ref=send.at[peer, part],
            dst_ref=recv.at[peer, part],
            send_sem=sent.at[peer],
            recv_sem=landed.at[peer],
            device_id=peer_id(peer, uly_count),
            device_id_type=MESH,
        )

    def dispatch_queries(step, carry):
        distance = count // 2 + (1 - 2 * (step % 2)) * ((step + 1) // 2)
        outward((me + distance) % count, query_part, q_send_sem, q_recv_sem).start()
        return carry

    lax.fori_loop(0, count - 1, dispatch_queries, 0)

    group = math.gcd(count, 8)
    group_count = count // group
    my_group = me // group
    if group_count == 4:
        near = my_group + 1 - 2 * (my_group % 2)
        planes = [my_group, near, (my_group + 2) % 4, 3 - my_group]
    else:
        planes = [(my_group + step) % group_count for step in range(group_count)]

    for plane in planes:

        def dispatch(step, carry, plane=plane):
            peer = plane * group + (step + me) % group

            @pl.when(peer != me)
            def _():
                outward(peer, kv_part, send_sem, recv_sem).start()

            return carry

        lax.fori_loop(0, group, dispatch, 0)

    def text_columns(text_in):
        return text_in[...].astype(jnp.float32).T

    loads[3].wait()
    loads[4].wait()
    both = jnp.concatenate(
        [unit_rows(text_columns(tk_in)) * tk_gain[...], text_columns(tv_in)], axis=-1
    )
    text_kv[...] = both.astype(jnp.bfloat16)
    loads[5].wait()
    text_probes = unit_rows(text_columns(tq_in)) * tq_gain[...] * my_sharp
    block = group * tokens
    queries[count * tokens :, :] = jnp.concatenate([text_probes, jnp.zeros_like(text_probes)], axis=-1).astype(
        jnp.bfloat16
    )
    bias = jnp.where(valid[...] == 1, 0.0, NEGATIVE)

    def with_ones(pairs):
        return jnp.where(lane_mask(pairs.shape, width), 1.0, pairs.astype(jnp.float32)).astype(
            jnp.bfloat16
        )

    def scores_of(rows, pairs):
        return lax.dot_general(
            rows, pairs, (((1,), (1,)), ((), ())), preferred_element_type=jnp.float32
        )

    def row_max(scores):
        return jnp.max(scores, axis=1, keepdims=True)

    def weighted(scores, peak, pairs):
        return jnp.dot(
            jnp.exp(scores - peak).astype(jnp.bfloat16), pairs, preferred_element_type=jnp.float32
        )

    def arrive_queries(step, carry):
        inward((me + 1 + step) % count, query_part, q_send_sem, q_recv_sem).wait_recv()
        return carry

    lax.fori_loop(0, count - 1, arrive_queries, 0)
    group_rows = group * half_tokens
    for index in range(group_count):
        packed = (
            recv[index * group : (index + 1) * group, tokens:, :]
            .reshape(group_rows, lanes)
            .astype(jnp.float32)
        )
        low = lane_mask(packed.shape, width)
        for side, rows in enumerate((packed, pltpu.roll(packed, width, 1))):
            start = index * block + side * group_rows
            queries[start : start + group_rows, :] = jnp.where(low, rows, 0.0).astype(jnp.bfloat16)

    def plane_pairs(plane):
        def arrive(step, carry):
            peer = plane * group + step

            @pl.when(peer != me)
            def _():
                inward(peer, kv_part, send_sem, recv_sem).wait_recv()

            return carry

        lax.fori_loop(0, group, arrive, 0)
        first = pl.multiple_of(plane * group, group)
        return recv[pl.ds(first, group), :tokens, :].reshape(block, lanes)

    block_count = group_count + text_tokens // block

    def block_rows(index):
        return pl.ds(pl.multiple_of(index * block, block), block)

    def fill(peak, scores):
        return jnp.concatenate([peak] * (scores.shape[1] // lanes), axis=1)

    def full_peak(scores):
        return jnp.broadcast_to(row_max(scores), (block, lanes))

    early = group_count // 2
    pairs = jnp.concatenate([text_kv[...]] + [plane_pairs(plane) for plane in planes[:early]], axis=0)
    ones = with_ones(pairs)
    wide_bias = jnp.concatenate([bias, jnp.zeros((1, early * block), jnp.float32)], axis=1)
    for index in range(block_count):
        scores = scores_of(queries[block_rows(index), :], pairs) + wide_bias
        peak = full_peak(scores)
        totals[block_rows(index), :] = weighted(scores, fill(peak, scores), ones)
        peaks[block_rows(index), :] = peak

    def absorb(index, pairs, ones):
        scores = scores_of(queries[block_rows(index), :], pairs)
        earlier = peaks[block_rows(index), :]
        peak = jnp.maximum(earlier, full_peak(scores))
        total = totals[block_rows(index), :] * jnp.exp(earlier - peak) + weighted(
            scores, fill(peak, scores), ones
        )
        return peak, total

    for plane in planes[early:-1]:
        pairs = plane_pairs(plane)
        ones = with_ones(pairs)
        for index in range(block_count):
            peak, total = absorb(index, pairs, ones)
            totals[block_rows(index), :] = total
            peaks[block_rows(index), :] = peak

    pairs = plane_pairs(planes[-1])
    ones = with_ones(pairs)

    def attend(index):
        _, total = absorb(index, pairs, ones)
        return total / pltpu.roll(total, width, 1)

    def pair_up(first, second):
        return jnp.where(lane_mask(first.shape, width), pltpu.roll(first, width, 1), second)

    def homeward(peer):
        return pltpu.make_async_remote_copy(
            src_ref=back_send.at[peer],
            dst_ref=back_out.at[me],
            send_sem=back_send_sem.at[peer],
            recv_sem=back_recv_sem.at[me],
            device_id=peer_id(peer, uly_count),
            device_id_type=MESH,
        )

    def returned(peer):
        return pltpu.make_async_remote_copy(
            src_ref=back_send.at[peer],
            dst_ref=back_out.at[peer],
            send_sem=back_send_sem.at[peer],
            recv_sem=back_recv_sem.at[peer],
            device_id=peer_id(peer, uly_count),
            device_id_type=MESH,
        )

    for which in planes[::-1]:
        first_peer = pl.multiple_of(which * group, group)
        attended = attend(which)
        back_send[pl.ds(first_peer, group)] = (
            pair_up(attended[:group_rows], attended[group_rows:])
            .astype(jnp.bfloat16)
            .reshape(group, half_tokens, lanes)
        )

        def hand_back(step, carry, first_peer=first_peer):
            peer = first_peer + (step + me) % group

            @pl.when(peer != me)
            def _():
                homeward(peer).start()

            return carry

        lax.fori_loop(0, group, hand_back, 0)
    own_back = pltpu.make_async_copy(back_send.at[me], back_out.at[me], own_sem.at[0])
    own_back.start()

    attended = jnp.concatenate(
        [attend(index) for index in range(group_count, block_count)], axis=0
    )
    turned = attended.T[width:]
    for part in range(uly_count):
        text_send[part] = turned[:, part * text_share : (part + 1) * text_share].astype(
            jnp.bfloat16
        )

    def text_copy(part, slot):
        return pltpu.make_async_remote_copy(
            src_ref=text_send.at[part],
            dst_ref=txt_out.at[slot],
            send_sem=text_send_sem.at[part],
            recv_sem=text_recv_sem.at[slot],
            device_id={"blk": my_blk, "uly": part},
            device_id_type=MESH,
        )

    for step in range(1, uly_count):
        text_copy((my_uly + step) % uly_count, my_uly).start()
    own_text = pltpu.make_async_copy(text_send.at[my_uly], txt_out.at[my_uly], own_sem.at[1])
    own_text.start()

    for step in range(1, uly_count):
        other = (my_uly + step) % uly_count
        text_copy(other, other).wait_recv()
    own_back.wait()
    own_text.wait()

    def collect(step, carry):
        returned((me + 1 + step) % count).wait_recv()
        return carry

    lax.fori_loop(0, count - 1, collect, 0)
    def drain(step, carry):
        peer = (me + 1 + step) % count
        outward(peer, query_part, q_send_sem, q_recv_sem).wait_send()
        outward(peer, kv_part, send_sem, recv_sem).wait_send()
        homeward(peer).wait_send()
        return carry

    lax.fori_loop(0, count - 1, drain, 0)
    for step in range(1, uly_count):
        text_copy((my_uly + step) % uly_count, my_uly).wait_send()


def lay_out_kernel(back_ref, txt_ref, vid_out, txt_out, wide):
    heads, half, lanes = back_ref.shape
    width = lanes // 2
    for head in range(heads):
        wide[:, head, :] = back_ref[head].astype(jnp.float32)
    vid_out[:half] = wide[:, :, :width].astype(jnp.bfloat16)
    vid_out[half:] = wide[:, :, width:].astype(jnp.bfloat16)
    txt_out[...] = txt_ref[...]


def fused_on_device(blk_count, uly_count, *operands):
    vq, vk, vv, tq, tk, tv, vq_gain, vk_gain, tq_gain, tk_gain, sharp, valid = operands
    tokens, heads, width = vq.shape
    text_tokens = tq.shape[0]
    count = blk_count * uly_count
    lanes = 2 * width
    text_share = text_tokens // uly_count
    half = tokens // 2
    bf16, f32 = jnp.bfloat16, jnp.float32
    any_spec = pl.BlockSpec(memory_space=pl.ANY)
    vmem_spec = pl.BlockSpec(memory_space=pltpu.VMEM)
    dma = pltpu.SemaphoreType.DMA
    text_shape = jax.ShapeDtypeStruct((uly_count, width, text_share), bf16)
    back, text_back = pl.pallas_call(
        functools.partial(fused_kernel, blk_count, uly_count),
        out_shape=(
            jax.ShapeDtypeStruct((count, half, lanes), bf16),
            text_shape,
        ),
        in_specs=[any_spec] * 12,
        out_specs=(any_spec, any_spec),
        scratch_shapes=[
            pltpu.VMEM((tokens, heads, width), bf16),
            pltpu.VMEM((tokens, heads, width), bf16),
            pltpu.VMEM((tokens, heads, width), bf16),
            pltpu.VMEM((width, text_tokens), bf16),
            pltpu.VMEM((width, text_tokens), bf16),
            pltpu.VMEM((width, text_tokens), bf16),
            pltpu.VMEM((1, width), f32),
            pltpu.VMEM((1, width), f32),
            pltpu.VMEM((1, width), f32),
            pltpu.VMEM((1, width), f32),
            pltpu.VMEM((1, heads), f32),
            pltpu.VMEM((1, text_tokens), jnp.int32),
            pltpu.VMEM((tokens, heads, lanes), f32),
            pltpu.VMEM((half, heads, lanes), f32),
            pltpu.VMEM((count, tokens + half, lanes), bf16),
            pltpu.VMEM((count, tokens + half, lanes), bf16),
            pltpu.VMEM((text_tokens, lanes), bf16),
            pltpu.VMEM((count * tokens + text_tokens, lanes), bf16),
            pltpu.VMEM((count * tokens + text_tokens, lanes), f32),
            pltpu.VMEM((count * tokens + text_tokens, lanes), f32),
            pltpu.VMEM((count, half, lanes), bf16),
            pltpu.VMEM((uly_count, width, text_share), bf16),
            dma((12,)),
            dma((2,)),
            dma((count,)),
            dma((count,)),
            dma((count,)),
            dma((count,)),
            dma((count,)),
            dma((count,)),
            dma((uly_count,)),
            dma((uly_count,)),
        ],
        compiler_params=pltpu.CompilerParams(collective_id=0, has_side_effects=True),
        name="joint_attention",
    )(
        vq,
        vk,
        vv,
        jnp.transpose(tq, (1, 2, 0)),
        jnp.transpose(tk, (1, 2, 0)),
        jnp.transpose(tv, (1, 2, 0)),
        vq_gain[None],
        vk_gain[None],
        tq_gain[None],
        tk_gain[None],
        sharp[None],
        valid[None],
    )
    vid_out, txt_out = pl.pallas_call(
        lay_out_kernel,
        out_shape=(jax.ShapeDtypeStruct((tokens, heads, width), bf16), text_shape),
        in_specs=[vmem_spec] * 2,
        out_specs=(vmem_spec, vmem_spec),
        scratch_shapes=[pltpu.VMEM((half, heads, lanes), f32)],
        name="lay_out",
    )(back, text_back)
    return vid_out, jnp.transpose(txt_out, (2, 0, 1))


def fits_fused(mesh, vq, tq):
    count = mesh.shape["blk"] * mesh.shape["uly"]
    tokens = vq.shape[0] // count
    return (
        vq.shape[1] == count
        and 2 * vq.shape[2] == 128
        and tokens % 32 == 0
        and tokens <= 64
        and count >= 2 * math.gcd(count, 8)
        and tq.shape[0] % (math.gcd(count, 8) * tokens) == 0
        and tq.shape[0] % (128 * mesh.shape["uly"]) == 0
    )


def solution(mesh):
    blk_count, uly_count = mesh.shape["blk"], mesh.shape["uly"]

    def run(*operands):
        body = on_device
        if fits_fused(mesh, operands[0], operands[3]):
            body = functools.partial(fused_on_device, blk_count, uly_count)
        split = P(("blk", "uly"), None, None)
        return jax.shard_map(
            body,
            mesh=mesh,
            in_specs=(split, split, split) + (P(),) * 9,
            out_specs=(split, P("uly", "blk", None)),
            check_vma=False,
        )(*operands)

    return run
```

```python
import functools
import math

import jax
import jax.numpy as jnp
from jax import lax
from jax.experimental import pallas as pl
from jax.experimental.pallas import tpu as pltpu
from jax.sharding import PartitionSpec as P

EPSILON = 1e-06
NEGATIVE = -1e30
MESH = pl.DeviceIdType.MESH


def normed(tensor, gain_vector, rescale_factor):
    widened = tensor.astype(jnp.float32)
    inverse = lax.rsqrt(jnp.mean(widened * widened, axis=-1, keepdims=True) + EPSILON)
    return (widened * inverse * gain_vector * rescale_factor).astype(jnp.bfloat16)


def fragment_contributions(queries, key_rows, value_rows, valid):
    scores = jnp.einsum("qhd,khd->hqk", queries, key_rows, preferred_element_type=jnp.float32)
    if valid is not None:
        scores = jnp.where(valid[None, None, :], scores, NEGATIVE)
    maxima = jnp.max(scores, axis=-1)
    weights = jnp.exp(scores - maxima[..., None])
    if valid is not None:
        weights = jnp.where(valid[None, None, :], weights, 0.0)
    totals = jnp.sum(weights, axis=-1)
    accum = jnp.einsum(
        "hqk,khd->hqd", weights, value_rows.astype(jnp.float32), precision=lax.Precision.HIGHEST
    )
    return (maxima, totals, accum)


def combine(earlier, later):
    max_one, total_one, accum_one = earlier
    max_two, total_two, accum_two = later
    merged_max = jnp.maximum(max_one, max_two)
    factor_one = jnp.exp(max_one - merged_max)
    factor_two = jnp.exp(max_two - merged_max)
    merged_total = total_one * factor_one + total_two * factor_two
    merged_accum = accum_one * factor_one[..., None] + accum_two * factor_two[..., None]
    return (merged_max, merged_total, merged_accum)


def on_device(
    footage_probes,
    footage_lookup_keys,
    footage_payload,
    caption_probes,
    caption_lookup_keys,
    caption_payload,
    footage_probes_amplitude,
    footage_keys_amplitude,
    caption_probes_amplitude,
    caption_keys_amplitude,
    focus_sharpness,
    caption_validity,
):
    channel_width = footage_probes.shape[2]
    rescale_factor = focus_sharpness[None, :, None] / math.sqrt(channel_width)
    q_norm = normed(footage_probes, footage_probes_amplitude, rescale_factor)
    k_norm = normed(footage_lookup_keys, footage_keys_amplitude, 1.0)
    q_local = lax.all_to_all(q_norm, "blk", split_axis=1, concat_axis=0, tiled=True)
    k_local = lax.all_to_all(k_norm, "blk", split_axis=1, concat_axis=0, tiled=True)
    v_local = lax.all_to_all(footage_payload, "blk", split_axis=1, concat_axis=0, tiled=True)
    local_heads = q_local.shape[1]
    head_start = lax.axis_index("blk") * local_heads
    local_scale = lax.dynamic_slice_in_dim(rescale_factor, head_start, local_heads, 1)
    text_q = normed(
        lax.dynamic_slice_in_dim(caption_probes, head_start, local_heads, 1),
        caption_probes_amplitude,
        local_scale,
    )
    text_k = normed(
        lax.dynamic_slice_in_dim(caption_lookup_keys, head_start, local_heads, 1),
        caption_keys_amplitude,
        1.0,
    )
    text_v = lax.dynamic_slice_in_dim(caption_payload, head_start, local_heads, 1)
    text_valid = caption_validity == 1
    text_share = caption_probes.shape[0] // lax.axis_size("uly")
    row_start = lax.axis_index("uly") * text_share
    video_rows = q_local.shape[0]
    queries = jnp.concatenate(
        [q_local, lax.dynamic_slice_in_dim(text_q, row_start, text_share, 0)], 0
    )

    def fold_inward(running, gathered):
        key_block, value_block = gathered
        row_count = key_block.shape[0]
        block_rows = math.gcd(row_count, 512)

        def absorb_block(block_index, running_state):
            key_part = lax.dynamic_slice_in_dim(key_block, block_index * block_rows, block_rows, 0)
            value_part = lax.dynamic_slice_in_dim(
                value_block, block_index * block_rows, block_rows, 0
            )
            return combine(
                running_state, fragment_contributions(queries, key_part, value_part, None)
            )

        return lax.fori_loop(0, row_count // block_rows, absorb_block, running)

    first_state = fragment_contributions(queries, text_k, text_v, text_valid)
    maxima, totals, accum = fold_inward(
        first_state,
        (
            lax.all_gather(k_local, "uly", axis=0, tiled=True),
            lax.all_gather(v_local, "uly", axis=0, tiled=True),
        ),
    )
    attended = jnp.transpose(accum / totals[..., None], (1, 0, 2)).astype(jnp.bfloat16)
    vid_out = lax.all_to_all(attended[:video_rows], "blk", split_axis=0, concat_axis=1, tiled=True)
    txt_out = attended[video_rows:]
    return (vid_out, txt_out)


def peer_id(flat, uly_count):
    return {"blk": flat // uly_count, "uly": flat % uly_count}


def lane_mask(shape, half):
    return lax.broadcasted_iota(jnp.int32, shape, len(shape) - 1) < half


def unit_rows(rows):
    return rows * lax.rsqrt(jnp.mean(rows * rows, axis=-1, keepdims=True) + EPSILON)


def fused_kernel(
    blk_count,
    uly_count,
    vq_hbm,
    vk_hbm,
    vv_hbm,
    tq_hbm,
    tk_hbm,
    tv_hbm,
    vq_gain_hbm,
    vk_gain_hbm,
    tq_gain_hbm,
    tk_gain_hbm,
    sharp_hbm,
    valid_hbm,
    back_out,
    txt_out,
    vq_in,
    vk_in,
    vv_in,
    tq_in,
    tk_in,
    tv_in,
    vq_gain,
    vk_gain,
    tq_gain,
    tk_gain,
    sharp,
    valid,
    kv_wide,
    q_wide,
    send,
    recv,
    text_kv,
    queries,
    totals,
    peaks,
    back_send,
    text_send,
    in_sem,
    own_sem,
    q_send_sem,
    q_recv_sem,
    send_sem,
    recv_sem,
    back_send_sem,
    back_recv_sem,
    text_send_sem,
    text_recv_sem,
):
    count = blk_count * uly_count
    my_blk = lax.axis_index("blk")
    my_uly = lax.axis_index("uly")
    me = my_blk * uly_count + my_uly
    tokens, heads, width = vq_in.shape
    half_tokens = tokens // 2
    _, text_tokens = tq_in.shape
    text_share = text_tokens // uly_count
    lanes = 2 * width

    barrier = pltpu.get_barrier_semaphore()

    def greet(step, carry):
        distance = count // 2 + (1 - 2 * (step % 2)) * ((step + 1) // 2)
        peer = (me + distance) % count
        pl.semaphore_signal(
            barrier, inc=1, device_id=peer_id(peer, uly_count), device_id_type=MESH
        )
        return carry

    lax.fori_loop(0, count - 1, greet, 0)

    loads = []
    for slot, (source, target) in enumerate(
        ((vk_hbm, vk_in), (vv_hbm, vv_in), (vq_hbm, vq_in))
    ):
        loads.append(pltpu.make_async_copy(source, target, in_sem.at[slot]))
    for slot, (source, target) in enumerate(
        ((tk_hbm, tk_in), (tv_hbm, tv_in), (tq_hbm, tq_in))
    ):
        loads.append(
            pltpu.make_async_copy(source.at[me], target, in_sem.at[3 + slot])
        )
    small = []
    for slot, (source, target) in enumerate(
        (
            (vk_gain_hbm, vk_gain),
            (vq_gain_hbm, vq_gain),
            (sharp_hbm, sharp),
            (tk_gain_hbm, tk_gain),
            (tq_gain_hbm, tq_gain),
            (valid_hbm, valid),
        )
    ):
        small.append(pltpu.make_async_copy(source, target, in_sem.at[6 + slot]))
    for load in small + loads:
        load.start()
    for load in small:
        load.wait()

    sharp_row = sharp[...] / math.sqrt(width)
    square = (heads, heads)
    sharp_column = jnp.sum(
        jnp.where(
            lax.broadcasted_iota(jnp.int32, square, 0) == lax.broadcasted_iota(jnp.int32, square, 1),
            jnp.broadcast_to(sharp_row, square),
            0.0,
        ),
        axis=1,
        keepdims=True,
    )
    my_sharp = jnp.sum(
        jnp.where(lax.broadcasted_iota(jnp.int32, (1, heads), 1) == me, sharp_row, 0.0),
        axis=1,
        keepdims=True,
    )

    loads[0].wait()
    loads[1].wait()
    keys = unit_rows(vk_in[...].astype(jnp.float32)) * vk_gain[...][None]
    kv_wide[...] = jnp.concatenate([keys, vv_in[...].astype(jnp.float32)], axis=-1)
    loads[2].wait()
    probes = unit_rows(vq_in[...].astype(jnp.float32)) * vq_gain[...][None] * sharp_column[None]
    q_wide[...] = jnp.concatenate([probes[:half_tokens], probes[half_tokens:]], axis=-1)
    for head in range(heads):
        send[head, :tokens, :] = kv_wide[:, head, :].astype(jnp.bfloat16)
        send[head, tokens:, :] = q_wide[:, head, :].astype(jnp.bfloat16)
    recv[me] = send[me]

    pl.semaphore_wait(barrier, count - 1)

    query_part, kv_part = pl.ds(tokens, half_tokens), pl.ds(0, tokens)

    def outward(peer, part, sent, landed):
        return pltpu.make_async_remote_copy(
            src_ref=send.at[peer, part],
            dst_ref=recv.at[me, part],
            send_sem=sent.at[peer],
            recv_sem=landed.at[me],
            device_id=peer_id(peer, uly_count),
            device_id_type=MESH,
        )

    def inward(peer, part, sent, landed):
        return pltpu.make_async_remote_copy(
            src_ref=send.at[peer, part],
            dst_ref=recv.at[peer, part],
            send_sem=sent.at[peer],
            recv_sem=landed.at[peer],
            device_id=peer_id(peer, uly_count),
            device_id_type=MESH,
        )

    def dispatch_queries(step, carry):
        distance = count // 2 + (1 - 2 * (step % 2)) * ((step + 1) // 2)
        outward((me + distance) % count, query_part, q_send_sem, q_recv_sem).start()
        return carry

    lax.fori_loop(0, count - 1, dispatch_queries, 0)

    group = math.gcd(count, 8)
    group_count = count // group
    my_group = me // group
    if group_count == 4:
        near = my_group + 1 - 2 * (my_group % 2)
        planes = [my_group, near, (my_group + 2) % 4, 3 - my_group]
    else:
        planes = [(my_group + step) % group_count for step in range(group_count)]

    for plane in planes:

        def dispatch(step, carry, plane=plane):
            peer = plane * group + (step + me) % group

            @pl.when(peer != me)
            def _():
                outward(peer, kv_part, send_sem, recv_sem).start()

            return carry

        lax.fori_loop(0, group, dispatch, 0)

    def text_columns(text_in):
        return text_in[...].astype(jnp.float32).T

    loads[3].wait()
    loads[4].wait()
    both = jnp.concatenate(
        [unit_rows(text_columns(tk_in)) * tk_gain[...], text_columns(tv_in)], axis=-1
    )
    text_kv[...] = both.astype(jnp.bfloat16)
    loads[5].wait()
    text_probes = unit_rows(text_columns(tq_in)) * tq_gain[...] * my_sharp
    block = group * tokens
    queries[count * tokens :, :] = jnp.concatenate([text_probes, jnp.zeros_like(text_probes)], axis=-1).astype(
        jnp.bfloat16
    )
    bias = jnp.where(valid[...] == 1, 0.0, NEGATIVE)

    def with_ones(pairs):
        return jnp.where(lane_mask(pairs.shape, width), 1.0, pairs.astype(jnp.float32)).astype(
            jnp.bfloat16
        )

    def scores_of(rows, pairs):
        return lax.dot_general(
            rows, pairs, (((1,), (1,)), ((), ())), preferred_element_type=jnp.float32
        )

    def row_max(scores):
        return jnp.max(scores, axis=1, keepdims=True)

    def weighted(scores, peak, pairs):
        return jnp.dot(
            jnp.exp(scores - peak).astype(jnp.bfloat16), pairs, preferred_element_type=jnp.float32
        )

    def arrive_queries(step, carry):
        inward((me + 1 + step) % count, query_part, q_send_sem, q_recv_sem).wait_recv()
        return carry

    lax.fori_loop(0, count - 1, arrive_queries, 0)
    group_rows = group * half_tokens
    for index in range(group_count):
        packed = (
            recv[index * group : (index + 1) * group, tokens:, :]
            .reshape(group_rows, lanes)
            .astype(jnp.float32)
        )
        low = lane_mask(packed.shape, width)
        for side, rows in enumerate((packed, pltpu.roll(packed, width, 1))):
            start = index * block + side * group_rows
            queries[start : start + group_rows, :] = jnp.where(low, rows, 0.0).astype(jnp.bfloat16)

    def plane_pairs(plane):
        def arrive(step, carry):
            peer = plane * group + step

            @pl.when(peer != me)
            def _():
                inward(peer, kv_part, send_sem, recv_sem).wait_recv()

            return carry

        lax.fori_loop(0, group, arrive, 0)
        first = pl.multiple_of(plane * group, group)
        return recv[pl.ds(first, group), :tokens, :].reshape(block, lanes)

    block_count = group_count + text_tokens // block

    def block_rows(index):
        return pl.ds(pl.multiple_of(index * block, block), block)

    def fill(peak, scores):
        return jnp.concatenate([peak] * (scores.shape[1] // lanes), axis=1)

    def full_peak(scores):
        return jnp.broadcast_to(row_max(scores), (block, lanes))

    early = group_count // 2
    pairs = jnp.concatenate([text_kv[...]] + [plane_pairs(plane) for plane in planes[:early]], axis=0)
    ones = with_ones(pairs)
    wide_bias = jnp.concatenate([bias, jnp.zeros((1, early * block), jnp.float32)], axis=1)
    for index in range(block_count):
        scores = scores_of(queries[block_rows(index), :], pairs) + wide_bias
        peak = full_peak(scores)
        totals[block_rows(index), :] = weighted(scores, fill(peak, scores), ones)
        peaks[block_rows(index), :] = peak

    def absorb(index, pairs, ones):
        scores = scores_of(queries[block_rows(index), :], pairs)
        earlier = peaks[block_rows(index), :]
        peak = jnp.maximum(earlier, full_peak(scores))
        total = totals[block_rows(index), :] * jnp.exp(earlier - peak) + weighted(
            scores, fill(peak, scores), ones
        )
        return peak, total

    for plane in planes[early:-1]:
        pairs = plane_pairs(plane)
        ones = with_ones(pairs)
        for index in range(block_count):
            peak, total = absorb(index, pairs, ones)
            totals[block_rows(index), :] = total
            peaks[block_rows(index), :] = peak

    pairs = plane_pairs(planes[-1])
    ones = with_ones(pairs)

    def attend(index):
        _, total = absorb(index, pairs, ones)
        return total / pltpu.roll(total, width, 1)

    def pair_up(first, second):
        return jnp.where(lane_mask(first.shape, width), pltpu.roll(first, width, 1), second)

    def homeward(peer):
        return pltpu.make_async_remote_copy(
            src_ref=back_send.at[peer],
            dst_ref=back_out.at[me],
            send_sem=back_send_sem.at[peer],
            recv_sem=back_recv_sem.at[me],
            device_id=peer_id(peer, uly_count),
            device_id_type=MESH,
        )

    def returned(peer):
        return pltpu.make_async_remote_copy(
            src_ref=back_send.at[peer],
            dst_ref=back_out.at[peer],
            send_sem=back_send_sem.at[peer],
            recv_sem=back_recv_sem.at[peer],
            device_id=peer_id(peer, uly_count),
            device_id_type=MESH,
        )

    for which in planes[::-1]:
        first_peer = pl.multiple_of(which * group, group)
        attended = attend(which)
        back_send[pl.ds(first_peer, group)] = (
            pair_up(attended[:group_rows], attended[group_rows:])
            .astype(jnp.bfloat16)
            .reshape(group, half_tokens, lanes)
        )

        def hand_back(step, carry, first_peer=first_peer):
            peer = first_peer + (step + me) % group

            @pl.when(peer != me)
            def _():
                homeward(peer).start()

            return carry

        lax.fori_loop(0, group, hand_back, 0)
    own_back = pltpu.make_async_copy(back_send.at[me], back_out.at[me], own_sem.at[0])
    own_back.start()

    attended = jnp.concatenate(
        [attend(index) for index in range(group_count, block_count)], axis=0
    )
    turned = attended.T[width:]
    for part in range(uly_count):
        text_send[part] = turned[:, part * text_share : (part + 1) * text_share].astype(
            jnp.bfloat16
        )

    def text_copy(part, slot):
        return pltpu.make_async_remote_copy(
            src_ref=text_send.at[part],
            dst_ref=txt_out.at[slot],
            send_sem=text_send_sem.at[part],
            recv_sem=text_recv_sem.at[slot],
            device_id={"blk": my_blk, "uly": part},
            device_id_type=MESH,
        )

    for step in range(1, uly_count):
        text_copy((my_uly + step) % uly_count, my_uly).start()
    own_text = pltpu.make_async_copy(text_send.at[my_uly], txt_out.at[my_uly], own_sem.at[1])
    own_text.start()

    for step in range(1, uly_count):
        other = (my_uly + step) % uly_count
        text_copy(other, other).wait_recv()
    own_back.wait()
    own_text.wait()

    def collect(step, carry):
        returned((me + 1 + step) % count).wait_recv()
        return carry

    lax.fori_loop(0, count - 1, collect, 0)
    def drain(step, carry):
        peer = (me + 1 + step) % count
        outward(peer, query_part, q_send_sem, q_recv_sem).wait_send()
        outward(peer, kv_part, send_sem, recv_sem).wait_send()
        homeward(peer).wait_send()
        return carry

    lax.fori_loop(0, count - 1, drain, 0)
    for step in range(1, uly_count):
        text_copy((my_uly + step) % uly_count, my_uly).wait_send()


def lay_out_kernel(back_ref, txt_ref, vid_out, txt_out, wide):
    heads, half, lanes = back_ref.shape
    width = lanes // 2
    for head in range(heads):
        wide[:, head, :] = back_ref[head].astype(jnp.float32)
    vid_out[:half] = wide[:, :, :width].astype(jnp.bfloat16)
    vid_out[half:] = wide[:, :, width:].astype(jnp.bfloat16)
    txt_out[...] = txt_ref[...]


def fused_on_device(blk_count, uly_count, *operands):
    vq, vk, vv, tq, tk, tv, vq_gain, vk_gain, tq_gain, tk_gain, sharp, valid = operands
    tokens, heads, width = vq.shape
    text_tokens = tq.shape[0]
    count = blk_count * uly_count
    lanes = 2 * width
    text_share = text_tokens // uly_count
    half = tokens // 2
    bf16, f32 = jnp.bfloat16, jnp.float32
    any_spec = pl.BlockSpec(memory_space=pl.ANY)
    vmem_spec = pl.BlockSpec(memory_space=pltpu.VMEM)
    dma = pltpu.SemaphoreType.DMA
    text_shape = jax.ShapeDtypeStruct((uly_count, width, text_share), bf16)
    back, text_back = pl.pallas_call(
        functools.partial(fused_kernel, blk_count, uly_count),
        out_shape=(
            jax.ShapeDtypeStruct((count, half, lanes), bf16),
            text_shape,
        ),
        in_specs=[any_spec] * 12,
        out_specs=(any_spec, any_spec),
        scratch_shapes=[
            pltpu.VMEM((tokens, heads, width), bf16),
            pltpu.VMEM((tokens, heads, width), bf16),
            pltpu.VMEM((tokens, heads, width), bf16),
            pltpu.VMEM((width, text_tokens), bf16),
            pltpu.VMEM((width, text_tokens), bf16),
            pltpu.VMEM((width, text_tokens), bf16),
            pltpu.VMEM((1, width), f32),
            pltpu.VMEM((1, width), f32),
            pltpu.VMEM((1, width), f32),
            pltpu.VMEM((1, width), f32),
            pltpu.VMEM((1, heads), f32),
            pltpu.VMEM((1, text_tokens), jnp.int32),
            pltpu.VMEM((tokens, heads, lanes), f32),
            pltpu.VMEM((half, heads, lanes), f32),
            pltpu.VMEM((count, tokens + half, lanes), bf16),
            pltpu.VMEM((count, tokens + half, lanes), bf16),
            pltpu.VMEM((text_tokens, lanes), bf16),
            pltpu.VMEM((count * tokens + text_tokens, lanes), bf16),
            pltpu.VMEM((count * tokens + text_tokens, lanes), f32),
            pltpu.VMEM((count * tokens + text_tokens, lanes), f32),
            pltpu.VMEM((count, half, lanes), bf16),
            pltpu.VMEM((uly_count, width, text_share), bf16),
            dma((12,)),
            dma((2,)),
            dma((count,)),
            dma((count,)),
            dma((count,)),
            dma((count,)),
            dma((count,)),
            dma((count,)),
            dma((uly_count,)),
            dma((uly_count,)),
        ],
        compiler_params=pltpu.CompilerParams(
            collective_id=0, has_side_effects=True, vmem_limit_bytes=64960 * 1024
        ),
        name="joint_attention",
    )(
        vq,
        vk,
        vv,
        jnp.transpose(tq, (1, 2, 0)),
        jnp.transpose(tk, (1, 2, 0)),
        jnp.transpose(tv, (1, 2, 0)),
        vq_gain[None],
        vk_gain[None],
        tq_gain[None],
        tk_gain[None],
        sharp[None],
        valid[None],
    )
    vid_out, txt_out = pl.pallas_call(
        lay_out_kernel,
        out_shape=(jax.ShapeDtypeStruct((tokens, heads, width), bf16), text_shape),
        in_specs=[vmem_spec] * 2,
        out_specs=(vmem_spec, vmem_spec),
        scratch_shapes=[pltpu.VMEM((half, heads, lanes), f32)],
        compiler_params=pltpu.CompilerParams(vmem_limit_bytes=8 * 1024 * 1024),
        name="lay_out",
    )(back, text_back)
    return vid_out, jnp.transpose(txt_out, (2, 0, 1))


def fits_fused(mesh, vq, tq):
    count = mesh.shape["blk"] * mesh.shape["uly"]
    tokens = vq.shape[0] // count
    return (
        vq.shape[1] == count
        and 2 * vq.shape[2] == 128
        and tokens % 32 == 0
        and tokens <= 64
        and count >= 2 * math.gcd(count, 8)
        and tq.shape[0] % (math.gcd(count, 8) * tokens) == 0
        and tq.shape[0] % (128 * mesh.shape["uly"]) == 0
    )


def solution(mesh):
    blk_count, uly_count = mesh.shape["blk"], mesh.shape["uly"]

    def run(*operands):
        body = on_device
        if fits_fused(mesh, operands[0], operands[3]):
            body = functools.partial(fused_on_device, blk_count, uly_count)
        split = P(("blk", "uly"), None, None)
        return jax.shard_map(
            body,
            mesh=mesh,
            in_specs=(split, split, split) + (P(),) * 9,
            out_specs=(split, P("uly", "blk", None)),
            check_vma=False,
        )(*operands)

    return run
```
